128 devices in a mesh: own: 32 (over x, z, core), rep: 4 (over y).
Axes of the slice: x: 4, y: 4, z: 4, core: 2. Of those that a mesh axis runs over, the one named last changes fastest.
Arguments:
- block_pool: bfloat16 [8192, 64, 576], P(('own', 'rep')), may hold values from -16 to 16
- sel_index: int32 [4096], P(('own', 'rep')), may hold values from 0 to 63
- sel_layer: int32 [4096], P(('own', 'rep')), may hold values from 0 to 15, as said below
- counts: int32 [128], P(('own', 'rep')), may hold values from 8 to 32, as said below
Outputs:
- quant_codes: bfloat16 [32, 4, 32, 8, 18432], P('own', 'rep')
- quant_steps: float32 [32, 288], P('own')
- clip_error: float32 [32, 288], P('own')
The draws below stay inside these ranges and needn't reach their ends.
Inputs may be any that keep to these rules, and one draw needn't show every extreme that they name: `sel_layer`: among the 32 entries of one device, at most 8 name any one layer; the first 8 entries of every device all name one and the same layer. `counts`: some device has all 32 entries live.
All inputs are finite; a program needn't handle non-finite values.
Results may differ from the reference program's by a relative error of at most 0.001.
Values may be sent and summed in bfloat16 or wider, within the bound.
A program may use at most 128 MiB of HBM per device.

```python
import math
import jax
import jax.numpy as jnp
from jax import lax

LATENT = 576
TOKB = 64
SLICES = 2
CAP = 8
POOL_DEV = 64
SEL_DEV = 32
LAYERS = 16
HALF = 288
SEL_ALL = 4096
N_OWN = 32
N_REP = 4


def draw_block_pool(key, part):
    base_key = jax.random.fold_in(key, 11)
    key_chan, key_base, key_rows = jax.random.split(base_key, 3)
    shape = (N_OWN * N_REP * POOL_DEV, TOKB, LATENT)
    channel = jnp.exp(jax.random.uniform(key_chan, (LATENT,), jnp.float32, math.log(0.3), math.log(3.0)))
    base = jnp.clip(jax.random.normal(key_base, shape, jnp.float32), -5.0, 5.0)
    row_scale = jnp.ones((shape[0], 1, 1), jnp.float32)
    return (base * channel * row_scale).astype(jnp.bfloat16)


def draw_sel_layer(key, part):
    devices = N_OWN * N_REP
    base_key = jax.random.fold_in(key, 31)
    key_star, key_perm = jax.random.split(base_key, 2)
    star_layer = jax.random.randint(key_star, (), 0, LAYERS)
    items = jnp.arange((LAYERS - 1) * CAP, dtype=jnp.int32) // CAP
    device_keys = jax.random.split(key_perm, devices)

    def per_device(device_key):
        shuffled = jax.random.permutation(device_key, items)[:SEL_DEV - CAP]
        others = (star_layer + 1 + shuffled) % LAYERS
        front = jnp.full((CAP,), star_layer, jnp.int32)
        return jnp.concatenate([front, others.astype(jnp.int32)])
    return jax.vmap(per_device)(device_keys).reshape(-1).astype(jnp.int32)


def draw_counts(key, part):
    devices = N_OWN * N_REP
    base_key = jax.random.fold_in(key, 21)
    key_low, key_full, key_first = jax.random.split(base_key, 3)
    lower = jax.random.randint(key_low, (devices,), CAP, CAP + (SEL_DEV - CAP) // 3 + 1)
    full_mask = jax.random.randint(key_full, (devices,), 0, 8) == 0
    first_full = jax.random.randint(key_first, (), 0, devices)
    full_mask = full_mask | (jnp.arange(devices) == first_full)
    return jnp.where(full_mask, SEL_DEV, lower).astype(jnp.int32)


def touch_ends(drawn, stream_key, low, high):
    index_at = [jax.random.randint(jax.random.fold_in(stream_key, axis), (), 0, length) for axis, length in enumerate(drawn.shape)]
    main_axis = drawn.shape.index(max(drawn.shape))
    neighbour = index_at[:main_axis] + [(index_at[main_axis] + 1) % drawn.shape[main_axis]] + index_at[main_axis + 1:]
    return drawn.at[tuple(index_at)].set(low).at[tuple(neighbour)].set(high)


def setup_inputs(seed: int = 0) -> dict:
    seeds = jax.random.split(jax.random.key(seed), 5)
    return {
        "block_pool": draw_block_pool(jax.random.fold_in(seeds[4], 71), 0),
        "sel_index": touch_ends(jax.random.randint(seeds[1], (SEL_ALL,), 0, POOL_DEV), jax.random.fold_in(seeds[1], 1), 0, POOL_DEV - 1).astype(jnp.int32),
        "sel_layer": draw_sel_layer(jax.random.fold_in(seeds[4], 71), 0),
        "counts": draw_counts(jax.random.fold_in(seeds[4], 71), 0),
    }


headroom = 0.5


def slot_table(index_row, layer_row, live_count, group_layer, capacity):
    n_select = index_row.shape[0]
    is_live = jnp.arange(n_select) < live_count
    matches = (layer_row[None, :] == group_layer[:, None]) & is_live[None, :]
    ranking = jnp.cumsum(matches.astype(jnp.int32), axis=1) - 1
    slot_hit = matches[:, None, :] & (ranking[:, None, :] == jnp.arange(capacity)[None, :, None])
    chosen = jnp.sum(jnp.where(slot_hit, index_row[None, None, :], 0), axis=2).astype(jnp.int32)
    filled = jnp.any(slot_hit, axis=2)
    return chosen, filled


def reference(block_pool, sel_index, sel_layer, counts):
    devices = N_OWN * N_REP
    group_layer = (jnp.arange(N_OWN) // SLICES).astype(jnp.int32)
    index_rows = sel_index.reshape(devices, SEL_DEV)
    layer_rows = sel_layer.reshape(devices, SEL_DEV)
    chosen, filled = jax.vmap(lambda a, b, c: slot_table(a, b, c, group_layer, CAP))(index_rows, layer_rows, counts)
    pools = block_pool.reshape(devices, POOL_DEV, TOKB, SLICES, HALF)
    device_ids = jnp.arange(devices)[:, None]
    denominator = float(N_OWN * N_REP * CAP * TOKB)

    def one_group(group):
        slice_of = group % SLICES
        picked = jnp.take(chosen, group, axis=1)
        keep_mask = jnp.take(filled, group, axis=1)
        blocks = pools[device_ids, picked, :, slice_of]
        blocks = jnp.where(keep_mask[:, :, None, None], blocks, jnp.zeros((), blocks.dtype))
        values = blocks.astype(jnp.float32)
        peak_abs = jnp.max(jnp.abs(values), axis=(0, 1, 2))
        step_size = headroom * jnp.maximum(peak_abs, 1.0) / 127.0
        encoded = jnp.clip(values / step_size, -127.0, 127.0).astype(jnp.bfloat16)
        encoded = lax.optimization_barrier(encoded)
        decoded = encoded.astype(jnp.float32) * step_size
        sq_error = jnp.sum((values - decoded) ** 2, axis=(0, 1, 2))
        error_out = sq_error / (step_size * step_size * denominator)
        codes_out = encoded.reshape(N_OWN, N_REP, CAP, TOKB * HALF).transpose(1, 0, 2, 3)
        return codes_out, step_size, error_out

    quant_codes, quant_steps, clip_error = lax.map(one_group, jnp.arange(N_OWN))
    return quant_codes, quant_steps, clip_error
```

```python
import functools
import math

import jax
import jax.numpy as jnp
from jax import lax
from jax.experimental import pallas as pl
from jax.experimental.pallas import tpu as pltpu
from jax.sharding import PartitionSpec as P

SLICES = 2
LANES = 128
headroom = 0.5


SIDE = 4
ROUNDS = (
    ((2, 2),), ((2, 0), (0, 2)), ((2, 1), (0, -1)), ((2, -1), (0, 1)),
    ((1, 2), (-1, 0)), ((-1, 2), (1, 0)), ((1, 1), (-1, -1)), ((1, -1), (-1, 1)),
)


def shifted_layer(my_layer, offset, sign=1):
    dx, dz = offset
    x = lax.rem(my_layer // SIDE + sign * dx + SIDE, SIDE)
    z = lax.rem(my_layer % SIDE + sign * dz + SIDE, SIDE)
    return x * SIDE + z


def fill_slots(live, index_row, layer_row, table, layers, cap, empty):
    n_select = index_row.shape[1]
    is_live = lax.broadcasted_iota(jnp.int32, (1, n_select), 1) < live
    before = lax.broadcasted_iota(jnp.int32, (n_select, n_select), 0)
    after = lax.broadcasted_iota(jnp.int32, (n_select, n_select), 1)
    earlier = jnp.where(before < after, 1.0, 0.0)
    wanted = lax.broadcasted_iota(jnp.int32, (layers, n_select), 0)
    matches = jnp.where((layer_row == wanted) & is_live, 1.0, 0.0)
    ranking = jnp.dot(matches, earlier, preferred_element_type=jnp.float32)
    slot = lax.broadcasted_iota(jnp.int32, (cap, n_select), 0).astype(jnp.float32)
    shifted = index_row.astype(jnp.float32) - float(empty)
    for layer in range(layers):
        hit = (ranking[layer:layer + 1] == slot) & (matches[layer:layer + 1] > 0.5)
        found = jnp.sum(jnp.where(hit, shifted, 0.0), axis=1, keepdims=True) + float(empty)
        table[layer * cap:(layer + 1) * cap, :] = jnp.broadcast_to(found, (cap, LANES)).astype(jnp.int32)


def kernel(own_n, rep_n, cap, live_ref, index_ref, layer_ref, pool_ref, codes_ref, steps_ref, err_ref,
           table, slots, pool_v, stage, send, recv, pk_send, pk_recv, pk_mine, pk_rep, er_mine, er_rep,
           table_sem, pool_sem, ssem, rsem, pssem, prsem, rpssem, rprsem, ressem, rersem):
    rows, tokens, width = pool_ref.shape
    half = width // SLICES
    flat = tokens * half
    group = LANES // math.gcd(half, LANES)
    period = group * half
    layers = own_n // SLICES
    me = lax.axis_index("own")
    rep = lax.axis_index("rep")
    my_layer = me // SLICES
    my_slice = me % SLICES
    tiles = stage.shape[0]
    denominator = float(own_n * rep_n * cap * tokens)
    pieces = pool_sem.shape[0]
    per_piece = rows // pieces

    loads = [
        pltpu.make_async_copy(
            pool_ref.at[pl.ds(p * per_piece, per_piece)],
            pool_v.at[pl.ds(p * per_piece, per_piece)],
            pool_sem.at[p],
        )
        for p in range(pieces)
    ]
    for load in loads:
        load.start()

    barrier = pltpu.get_barrier_semaphore()
    for k in range(1, own_n):
        pl.semaphore_signal(barrier, inc=1, device_id={"own": lax.rem(me + k, own_n)},
                            device_id_type=pl.DeviceIdType.MESH)
    for k in range(1, rep_n):
        pl.semaphore_signal(barrier, inc=1, device_id={"rep": lax.rem(rep + k, rep_n)},
                            device_id_type=pl.DeviceIdType.MESH)

    pool_v[rows] = jnp.zeros((tokens, width), pool_v.dtype)
    fill_slots(live_ref[0], index_ref[...], layer_ref[...], table, layers, cap, rows)
    to_scalars = pltpu.make_async_copy(table, slots, table_sem)
    to_scalars.start()
    to_scalars.wait()
    for load in loads:
        load.wait()

    def row_of(slot):
        return jnp.minimum(jnp.maximum(slots[slot, 0], 0), rows)

    def layer_peak(layer, carry):
        best = jnp.zeros((tokens, width), pool_v.dtype)
        for c in range(cap):
            best = jnp.maximum(best, jnp.abs(pool_v[row_of(layer * cap + c)]))
        top = jnp.max(best.astype(jnp.float32), axis=0, keepdims=True)
        for part in range(SLICES):
            one = top[:, part * half:(part + 1) * half]
            pk_send[layer * SLICES + part] = jnp.concatenate([one] * group, axis=1)
        return carry

    def peak_copy(peer, landing):
        return pltpu.make_async_remote_copy(
            src_ref=pk_send.at[peer], dst_ref=pk_recv.at[landing],
            send_sem=pssem.at[peer], recv_sem=prsem.at[landing],
            device_id={"own": peer}, device_id_type=pl.DeviceIdType.MESH)

    def block_copy(peer, landing):
        return pltpu.make_async_remote_copy(
            src_ref=send.at[peer], dst_ref=recv.at[landing],
            send_sem=ssem.at[peer], recv_sem=rsem.at[landing],
            device_id={"own": peer}, device_id_type=pl.DeviceIdType.MESH)

    def flatten_layer(layer):
        for c in range(cap):
            block = pool_v[row_of(layer * cap + c)].astype(jnp.float32)
            for q in range(tiles):
                lo, hi = q * LANES, min(width, (q + 1) * LANES)
                stage[q, c * tokens:(c + 1) * tokens, 0:hi - lo] = block[:, lo:hi]

        def flatten(i, carry):
            rows_of = [
                jnp.concatenate(
                    [stage[q, pl.ds(i * group + j, cap, stride=tokens), :] for q in range(tiles)], axis=1)
                for j in range(group)
            ]
            for part in range(SLICES):
                joined = jnp.concatenate([r[:, part * half:(part + 1) * half] for r in rows_of], axis=1)
                at = pl.multiple_of(i * period, period)
                send[layer * SLICES + part, :, pl.ds(at, period)] = joined.astype(send.dtype)
            return carry

        lax.fori_loop(0, tokens // group, flatten, 0)

    def peer_of(offset, part, sign=1):
        return shifted_layer(my_layer, offset, sign) * SLICES + lax.rem(my_slice + part, SLICES)

    def flatten_to(*offsets):
        for offset in offsets:
            flatten_layer(shifted_layer(my_layer, offset))

    def send_to(*offsets):
        for part in range(SLICES):
            for offset in offsets:
                if offset != (0, 0) or part:
                    block_copy(peer_of(offset, part), me).start()

    sent = set()

    def sent_to(offset, parts=range(SLICES)):
        for part in parts:
            block_copy(peer_of(offset, part), me).wait_send()
            sent.add((offset, part))

    flatten_to((2, 2))
    pl.semaphore_wait(barrier, own_n - 1 + rep_n - 1)
    send_to((2, 2))
    lax.fori_loop(0, layers, layer_peak, 0)
    for step in range(1, own_n):
        peak_copy(lax.rem(me + step, own_n), me).start()
    for offset in ((2, 0), (2, 1), (2, -1), (0, 0)):
        flatten_to(offset)
        send_to(offset)
    flatten_to((0, 2))
    sent_to((2, 2))
    send_to((0, 2))
    flatten_to((0, -1), (0, 1))
    for around in ROUNDS[4:]:
        flatten_to(*around)
    sent_to((2, 0))
    send_to((0, -1))

    best = pk_send[me]
    for k in range(1, own_n):
        src = lax.rem(me + k, own_n)
        peak_copy(src, src).wait_recv()
        best = jnp.maximum(best, pk_recv[src])
    pk_mine[...] = best

    def rep_copy(mine, table, s_sem, r_sem, peer, landing):
        return pltpu.make_async_remote_copy(
            src_ref=mine, dst_ref=table.at[landing],
            send_sem=s_sem.at[peer], recv_sem=r_sem.at[landing],
            device_id={"rep": peer}, device_id_type=pl.DeviceIdType.MESH)

    for k in range(1, rep_n):
        rep_copy(pk_mine, pk_rep, rpssem, rprsem, lax.rem(rep + k, rep_n), rep).start()
    for k in range(1, rep_n):
        src = lax.rem(rep + k, rep_n)
        rep_copy(pk_mine, pk_rep, rpssem, rprsem, src, src).wait_recv()
        best = jnp.maximum(best, pk_rep[src])

    step = headroom * jnp.maximum(best, 1.0) / 127.0
    inverse = 1.0 / step
    steps_ref[...] = step[:, :half]
    step_wide = jnp.broadcast_to(step, (cap, period))
    inv_wide = jnp.broadcast_to(inverse, (cap, period))

    def encode(source, src, total):
        def one(i, total):
            at = pl.multiple_of(i * period, period)
            x = source[src, :, pl.ds(at, period)].astype(jnp.float32)
            y = jnp.clip(x * inv_wide, -127.0, 127.0).astype(codes_ref.dtype)
            codes_ref[0, 0, src, :, pl.ds(at, period)] = y
            diff = x - y.astype(jnp.float32) * step_wide
            return total + diff * diff
        return lax.fori_loop(0, tokens // group, one, total)

    def take(offset, total):
        for part in range(SLICES):
            src = peer_of(offset, part, -1)
            block_copy(src, src).wait_recv()
            total = encode(recv, src, total)
        return total

    total = encode(send, me, jnp.zeros((cap, period), jnp.float32))
    src = peer_of((0, 0), 1)
    block_copy(src, src).wait_recv()
    total = encode(recv, src, total)
    total = take((2, 2), total)
    sent_to((2, 1))
    send_to((0, 1))
    total = take((2, 0), total)
    total = take((0, 2), total)
    sent_to((2, -1), (0,))
    for around in ROUNDS[4:]:
        send_to(*around)
    for around in ROUNDS[2:]:
        for offset in around:
            total = take(offset, total)

    mine = jnp.sum(total, axis=0, keepdims=True)
    er_mine[...] = mine
    for k in range(1, rep_n):
        rep_copy(er_mine, er_rep, ressem, rersem, lax.rem(rep + k, rep_n), rep).start()
    er_rep[rep] = mine
    for k in range(1, rep_n):
        src = lax.rem(rep + k, rep_n)
        rep_copy(er_mine, er_rep, ressem, rersem, src, src).wait_recv()
    whole = er_rep[0]
    for k in range(1, rep_n):
        whole = whole + er_rep[k]
    folded = whole[:, :half]
    for j in range(1, group):
        folded = folded + whole[:, j * half:(j + 1) * half]
    narrow = step[:, :half]
    err_ref[...] = folded / (narrow * narrow * denominator)

    for k in range(1, own_n):
        peak_copy(lax.rem(me + k, own_n), me).wait_send()
    for offset in ((0, 0),) + sum(ROUNDS, ()):
        for part in range(SLICES):
            if (offset, part) not in sent and (offset, part) != ((0, 0), 0):
                block_copy(peer_of(offset, part), me).wait_send()
    for k in range(1, rep_n):
        peer = lax.rem(rep + k, rep_n)
        rep_copy(pk_mine, pk_rep, rpssem, rprsem, peer, rep).wait_send()
        rep_copy(er_mine, er_rep, ressem, rersem, peer, rep).wait_send()


def write_out(codes_v, steps_v, err_v, codes_ref, steps_ref, err_ref, sems):
    own_n = codes_v.shape[2]
    moves = [pltpu.make_async_copy(codes_v.at[0, 0, src], codes_ref.at[0, 0, src], sems.at[src])
             for src in range(own_n)]
    moves.append(pltpu.make_async_copy(steps_v, steps_ref, sems.at[own_n]))
    moves.append(pltpu.make_async_copy(err_v, err_ref, sems.at[own_n + 1]))
    for move in moves:
        move.start()
    for move in moves:
        move.wait()


def body(block_pool, sel_index, sel_layer, counts):
    own_n = lax.axis_size("own")
    rep_n = lax.axis_size("rep")
    cap = sel_index.shape[0] // 4
    rows, tokens, width = block_pool.shape
    half = width // SLICES
    flat = tokens * half
    group = LANES // math.gcd(half, LANES)
    period = group * half
    layers = own_n // SLICES
    f32 = jnp.float32
    dma = pltpu.SemaphoreType.DMA
    dtype = block_pool.dtype
    codes, steps, err = pl.pallas_call(
        functools.partial(kernel, own_n, rep_n, cap),
        out_shape=(
            pltpu.VMEM((1, 1, own_n, cap, flat), dtype),
            pltpu.VMEM((1, half), f32),
            pltpu.VMEM((1, half), f32),
        ),
        in_specs=[
            pl.BlockSpec(memory_space=pltpu.SMEM), pl.BlockSpec(memory_space=pltpu.VMEM),
            pl.BlockSpec(memory_space=pltpu.VMEM), pl.BlockSpec(memory_space=pltpu.HBM)],
        out_specs=(
            pl.BlockSpec(memory_space=pltpu.VMEM),
            pl.BlockSpec(memory_space=pltpu.VMEM),
            pl.BlockSpec(memory_space=pltpu.VMEM),
        ),
        scratch_shapes=[
            pltpu.VMEM((layers * cap, LANES), jnp.int32),
            pltpu.SMEM((layers * cap, LANES), jnp.int32),
            pltpu.VMEM((rows + 1, tokens, width), dtype),
            pltpu.VMEM((pl.cdiv(width, LANES), cap * tokens, LANES), f32),
            pltpu.VMEM((own_n, cap, flat), dtype),
            pltpu.VMEM((own_n, cap, flat), dtype),
            pltpu.VMEM((own_n, 1, period), f32),
            pltpu.VMEM((own_n, 1, period), f32),
            pltpu.VMEM((1, period), f32),
            pltpu.VMEM((rep_n, 1, period), f32),
            pltpu.VMEM((1, period), f32),
            pltpu.VMEM((rep_n, 1, period), f32),
            dma, dma((8,)),
            dma((own_n,)), dma((own_n,)), dma((own_n,)), dma((own_n,)),
            dma((rep_n,)), dma((rep_n,)), dma((rep_n,)), dma((rep_n,)),
        ],
        compiler_params=pltpu.CompilerParams(
            collective_id=0, has_side_effects=True, vmem_limit_bytes=(63 * 1024 * 1024 - own_n * cap * flat * 2)),
        name="latent_code",
    )(counts, sel_index[None], sel_layer[None], block_pool)
    hbm = pl.BlockSpec(memory_space=pltpu.HBM)
    return pl.pallas_call(
        write_out,
        out_shape=tuple(jax.ShapeDtypeStruct(x.shape, x.dtype) for x in (codes, steps, err)),
        in_specs=[pl.BlockSpec(memory_space=pltpu.VMEM)] * 3,
        out_specs=(hbm, hbm, hbm),
        scratch_shapes=[dma((own_n + 2,))],
        compiler_params=pltpu.CompilerParams(vmem_limit_bytes=4 * 1024 * 1024),
        name="write_out",
    )(codes, steps, err)


def solution(mesh):
    return jax.shard_map(
        body,
        mesh=mesh,
        in_specs=(
            P(("own", "rep"), None, None),
            P(("own", "rep")),
            P(("own", "rep")),
            P(("own", "rep")),
        ),
        out_specs=(P("own", "rep", None, None, None), P("own", None), P("own", None)),
        check_vma=False,
    )
```

```python
import functools
import math

import jax
import jax.numpy as jnp
from jax import lax
from jax.experimental import pallas as pl
from jax.experimental.pallas import tpu as pltpu
from jax.sharding import PartitionSpec as P

SLICES = 2
LANES = 128
headroom = 0.5


SIDE = 4
ROUNDS = (
    ((2, 2),), ((2, 0), (0, 2)), ((2, 1), (0, -1)), ((2, -1), (0, 1)),
    ((1, 2), (-1, 0)), ((-1, 2), (1, 0)), ((1, 1), (-1, -1)), ((1, -1), (-1, 1)),
)


def shifted_layer(my_layer, offset, sign=1):
    dx, dz = offset
    x = lax.rem(my_layer // SIDE + sign * dx + SIDE, SIDE)
    z = lax.rem(my_layer % SIDE + sign * dz + SIDE, SIDE)
    return x * SIDE + z


def fill_slots(live, index_row, layer_row, layers, cap, empty):
    n_select = index_row.shape[1]
    before = lax.broadcasted_iota(jnp.int32, (n_select, n_select), 1)
    after = lax.broadcasted_iota(jnp.int32, (n_select, n_select), 0)
    same = before == after
    layer_col = jnp.sum(jnp.where(same, layer_row, 0), axis=1, keepdims=True)
    index_col = jnp.sum(jnp.where(same, index_row, 0), axis=1, keepdims=True)
    is_live = lax.broadcasted_iota(jnp.int32, (n_select, 1), 0) < live
    earlier = jnp.where(before < after, 1.0, 0.0)
    wanted = lax.broadcasted_iota(jnp.int32, (n_select, LANES), 1)
    matches = jnp.where((layer_col == wanted) & is_live, 1.0, 0.0)
    ranking = jnp.dot(earlier, matches, preferred_element_type=jnp.float32)
    shifted = index_col.astype(jnp.float32) - float(empty)
    rows = []
    for slot in range(cap):
        hit = (ranking == float(slot)) & (matches > 0.5)
        rows.append(jnp.sum(jnp.where(hit, shifted, 0.0), axis=0, keepdims=True) + float(empty))
    return jnp.concatenate(rows, axis=0).astype(jnp.int32)


def kernel(own_n, rep_n, cap, counts_hbm, index_hbm, layer_hbm, pool_ref, codes_ref, steps_ref, err_ref,
           live_ref, index_ref, layer_ref, table, slots, pool_v, stage, send, recv, pk_send, pk_recv, pk_mine, pk_rep, er_mine, er_rep,
           table_sem, small_sem, pool_sem, ssem, rsem, pssem, prsem, rpssem, rprsem, ressem, rersem):
    rows, tokens, width = pool_ref.shape
    half = width // SLICES
    flat = tokens * half
    group = LANES // math.gcd(half, LANES)
    period = group * half
    layers = own_n // SLICES
    me = lax.axis_index("own")
    rep = lax.axis_index("rep")
    my_layer = me // SLICES
    my_slice = me % SLICES
    tiles = stage.shape[0]
    denominator = float(own_n * rep_n * cap * tokens)
    pieces = pool_sem.shape[0]
    per_piece = rows // pieces

    small = [
        pltpu.make_async_copy(src, dst, small_sem.at[i])
        for i, (src, dst) in enumerate(((counts_hbm, live_ref), (index_hbm, index_ref), (layer_hbm, layer_ref)))
    ]
    loads = [
        pltpu.make_async_copy(
            pool_ref.at[pl.ds(p * per_piece, per_piece)],
            pool_v.at[pl.ds(p * per_piece, per_piece)],
            pool_sem.at[p],
        )
        for p in range(pieces)
    ]

    def peer_of(offset, part, sign=1):
        return shifted_layer(my_layer, offset, sign) * SLICES + lax.rem(my_slice + part, SLICES)

    for load in small + loads:
        load.start()

    barrier = pltpu.get_barrier_semaphore()
    for offset in sum(ROUNDS, ()):
        for part in range(SLICES):
            pl.semaphore_signal(barrier, inc=1, device_id={"own": peer_of(offset, part)},
                                device_id_type=pl.DeviceIdType.MESH)
    for part in range(1, SLICES):
        pl.semaphore_signal(barrier, inc=1, device_id={"own": peer_of((0, 0), part)},
                            device_id_type=pl.DeviceIdType.MESH)
    for k in range(1, rep_n):
        pl.semaphore_signal(barrier, inc=1, device_id={"rep": lax.rem(rep + k, rep_n)},
                            device_id_type=pl.DeviceIdType.MESH)
    pool_v[rows] = jnp.zeros((tokens, width), pool_v.dtype)
    for load in small:
        load.wait()
    table[...] = fill_slots(live_ref[0], index_ref[...], layer_ref[...], layers, cap, rows)
    to_scalars = pltpu.make_async_copy(table, slots, table_sem)
    to_scalars.start()
    to_scalars.wait()
    for load in loads:
        load.wait()

    def row_of(layer, c):
        return jnp.minimum(jnp.maximum(slots[c, layer], 0), rows)

    def layer_peak(layer, carry):
        best = jnp.zeros((tokens, width), pool_v.dtype)
        for c in range(cap):
            best = jnp.maximum(best, jnp.abs(pool_v[row_of(layer, c)]))
        top = jnp.max(best.astype(jnp.float32), axis=0, keepdims=True)
        for part in range(SLICES):
            one = top[:, part * half:(part + 1) * half]
            pk_send[layer * SLICES + part] = one
        return carry

    def peak_copy(peer, landing):
        return pltpu.make_async_remote_copy(
            src_ref=pk_send.at[peer], dst_ref=pk_recv.at[landing],
            send_sem=pssem.at[peer], recv_sem=prsem.at[landing],
            device_id={"own": peer}, device_id_type=pl.DeviceIdType.MESH)

    def block_copy(peer, landing):
        return pltpu.make_async_remote_copy(
            src_ref=send.at[peer], dst_ref=recv.at[landing],
            send_sem=ssem.at[peer], recv_sem=rsem.at[landing],
            device_id={"own": peer}, device_id_type=pl.DeviceIdType.MESH)

    def flatten_layer(layer):
        for c in range(cap):
            block = pool_v[row_of(layer, c)].astype(jnp.float32)
            for q in range(tiles):
                lo, hi = q * LANES, min(width, (q + 1) * LANES)
                stage[q, c * tokens:(c + 1) * tokens, 0:hi - lo] = block[:, lo:hi]

        def flatten(i, carry):
            rows_of = [
                jnp.concatenate(
                    [stage[q, pl.ds(i * group + j, cap, stride=tokens), :] for q in range(tiles)], axis=1)
                for j in range(group)
            ]
            for part in range(SLICES):
                joined = jnp.concatenate([r[:, part * half:(part + 1) * half] for r in rows_of], axis=1)
                at = pl.multiple_of(i * period, period)
                send[layer * SLICES + part, :, pl.ds(at, period)] = joined.astype(send.dtype)
            return carry

        lax.fori_loop(0, tokens // group, flatten, 0)

    def flatten_to(*offsets):
        for offset in offsets:
            flatten_layer(shifted_layer(my_layer, offset))

    def send_to(*offsets):
        for part in range(SLICES):
            for offset in offsets:
                if offset != (0, 0) or part:
                    block_copy(peer_of(offset, part), me).start()

    sent = set()

    def sent_to(offset, parts=range(SLICES)):
        for part in parts:
            block_copy(peer_of(offset, part), me).wait_send()
            sent.add((offset, part))

    def rep_copy(mine, table, s_sem, r_sem, peer, landing):
        return pltpu.make_async_remote_copy(
            src_ref=mine, dst_ref=table.at[landing],
            send_sem=s_sem.at[peer], recv_sem=r_sem.at[landing],
            device_id={"rep": peer}, device_id_type=pl.DeviceIdType.MESH)

    flatten_to((2, 2))
    pl.semaphore_wait(barrier, own_n - 1 + rep_n - 1)
    send_to((2, 2))
    lax.fori_loop(0, layers, layer_peak, 0)
    for step in range(1, own_n):
        peak_copy(lax.rem(me + step, own_n), me).start()
    for offset in ((2, 0), (2, 1), (2, -1), (0, 0)):
        flatten_to(offset)
        send_to(offset)
    flatten_to((0, 2))
    sent_to((2, 2))
    send_to((0, 2))
    flatten_to((0, -1), (0, 1), (1, 2), (-1, 0), (-1, 2), (1, 0))
    sent_to((2, 0))
    send_to((0, -1))

    best = pk_send[me]
    for k in range(1, own_n):
        src = lax.rem(me + k, own_n)
        peak_copy(src, src).wait_recv()
        best = jnp.maximum(best, pk_recv[src])
    pk_mine[...] = best
    for k in range(1, rep_n):
        rep_copy(pk_mine, pk_rep, rpssem, rprsem, lax.rem(rep + k, rep_n), rep).start()
    flatten_to((1, 1), (-1, -1), (1, -1), (-1, 1))
    for k in range(1, rep_n):
        src = lax.rem(rep + k, rep_n)
        rep_copy(pk_mine, pk_rep, rpssem, rprsem, src, src).wait_recv()
        best = jnp.maximum(best, pk_rep[src])

    narrow = headroom * jnp.maximum(best, 1.0) / 127.0
    steps_ref[...] = narrow
    step = jnp.concatenate([narrow] * group, axis=1)
    inverse = 1.0 / step
    step_wide = jnp.broadcast_to(step, (cap, period))
    inv_wide = jnp.broadcast_to(inverse, (cap, period))

    def encode(source, src, total):
        def one(i, total):
            at = pl.multiple_of(i * period, period)
            x = source[src, :, pl.ds(at, period)].astype(jnp.float32)
            y = jnp.clip(x * inv_wide, -127.0, 127.0).astype(codes_ref.dtype)
            codes_ref[0, 0, src, :, pl.ds(at, period)] = y
            diff = x - y.astype(jnp.float32) * step_wide
            return total + diff * diff
        return lax.fori_loop(0, tokens // group, one, total)

    def take(total, *offsets):
        for part in range(SLICES):
            for offset in offsets:
                src = peer_of(offset, part, -1)
                block_copy(src, src).wait_recv()
                total = encode(recv, src, total)
        return total

    total = encode(send, me, jnp.zeros((cap, period), jnp.float32))
    src = peer_of((0, 0), 1)
    block_copy(src, src).wait_recv()
    total = encode(recv, src, total)
    total = take(total, (2, 2))
    total = take(total, (2, 0))
    sent_to((2, 1))
    send_to((0, 1))
    total = take(total, (0, 2))
    sent_to((2, -1))
    for around in ROUNDS[4:]:
        send_to(*around)
    for around in ROUNDS[2:]:
        total = take(total, *around)

    mine = jnp.sum(total, axis=0, keepdims=True)
    er_mine[...] = mine
    for k in range(1, rep_n):
        rep_copy(er_mine, er_rep, ressem, rersem, lax.rem(rep + k, rep_n), rep).start()
    er_rep[rep] = mine
    for k in range(1, rep_n):
        src = lax.rem(rep + k, rep_n)
        rep_copy(er_mine, er_rep, ressem, rersem, src, src).wait_recv()
    whole = er_rep[0]
    for k in range(1, rep_n):
        whole = whole + er_rep[k]
    folded = whole[:, :half]
    for j in range(1, group):
        folded = folded + whole[:, j * half:(j + 1) * half]
    err_ref[...] = folded / (narrow * narrow * denominator)

    for k in range(1, own_n):
        peak_copy(lax.rem(me + k, own_n), me).wait_send()
    for offset in ((0, 0),) + sum(ROUNDS, ()):
        for part in range(SLICES):
            if (offset, part) not in sent and (offset, part) != ((0, 0), 0):
                block_copy(peer_of(offset, part), me).wait_send()
    for k in range(1, rep_n):
        peer = lax.rem(rep + k, rep_n)
        rep_copy(pk_mine, pk_rep, rpssem, rprsem, peer, rep).wait_send()
        rep_copy(er_mine, er_rep, ressem, rersem, peer, rep).wait_send()


def write_out(codes_v, steps_v, err_v, codes_ref, steps_ref, err_ref, sems):
    own_n = codes_v.shape[2]
    moves = [pltpu.make_async_copy(codes_v.at[0, 0, src], codes_ref.at[0, 0, src], sems.at[src])
             for src in range(own_n)]
    moves.append(pltpu.make_async_copy(steps_v, steps_ref, sems.at[own_n]))
    moves.append(pltpu.make_async_copy(err_v, err_ref, sems.at[own_n + 1]))
    for move in moves:
        move.start()
    for move in moves:
        move.wait()


def body(block_pool, sel_index, sel_layer, counts):
    own_n = lax.axis_size("own")
    rep_n = lax.axis_size("rep")
    cap = sel_index.shape[0] // 4
    rows, tokens, width = block_pool.shape
    half = width // SLICES
    flat = tokens * half
    group = LANES // math.gcd(half, LANES)
    period = group * half
    layers = own_n // SLICES
    f32 = jnp.float32
    dma = pltpu.SemaphoreType.DMA
    dtype = block_pool.dtype
    codes, steps, err = pl.pallas_call(
        functools.partial(kernel, own_n, rep_n, cap),
        out_shape=(
            pltpu.VMEM((1, 1, own_n, cap, flat), dtype),
            pltpu.VMEM((1, half), f32),
            pltpu.VMEM((1, half), f32),
        ),
        in_specs=[pl.BlockSpec(memory_space=pltpu.HBM)] * 4,
        out_specs=(
            pl.BlockSpec(memory_space=pltpu.VMEM),
            pl.BlockSpec(memory_space=pltpu.VMEM),
            pl.BlockSpec(memory_space=pltpu.VMEM),
        ),
        scratch_shapes=[
            pltpu.SMEM((1,), jnp.int32),
            pltpu.VMEM((1, sel_index.shape[0]), jnp.int32),
            pltpu.VMEM((1, sel_layer.shape[0]), jnp.int32),
            pltpu.VMEM((cap, LANES), jnp.int32),
            pltpu.SMEM((cap, LANES), jnp.int32),
            pltpu.VMEM((rows + 1, tokens, width), dtype),
            pltpu.VMEM((pl.cdiv(width, LANES), cap * tokens, LANES), f32),
            pltpu.VMEM((own_n, cap, flat), dtype),
            pltpu.VMEM((own_n, cap, flat), dtype),
            pltpu.VMEM((own_n, 1, half), f32),
            pltpu.VMEM((own_n, 1, half), f32),
            pltpu.VMEM((1, half), f32),
            pltpu.VMEM((rep_n, 1, half), f32),
            pltpu.VMEM((1, period), f32),
            pltpu.VMEM((rep_n, 1, period), f32),
            dma, dma((3,)), dma((8,)),
            dma((own_n,)), dma((own_n,)), dma((own_n,)), dma((own_n,)),
            dma((rep_n,)), dma((rep_n,)), dma((rep_n,)), dma((rep_n,)),
        ],
        compiler_params=pltpu.CompilerParams(
            collective_id=0, has_side_effects=True, vmem_limit_bytes=(63 * 1024 * 1024 - own_n * cap * flat * 2)),
        name="latent_code",
    )(counts, sel_index[None], sel_layer[None], block_pool)
    hbm = pl.BlockSpec(memory_space=pltpu.HBM)
    return pl.pallas_call(
        write_out,
        out_shape=tuple(jax.ShapeDtypeStruct(x.shape, x.dtype) for x in (codes, steps, err)),
        in_specs=[pl.BlockSpec(memory_space=pltpu.VMEM)] * 3,
        out_specs=(hbm, hbm, hbm),
        scratch_shapes=[dma((own_n + 2,))],
        compiler_params=pltpu.CompilerParams(vmem_limit_bytes=4 * 1024 * 1024),
        name="write_out",
    )(codes, steps, err)


def solution(mesh):
    return jax.shard_map(
        body,
        mesh=mesh,
        in_specs=(
            P(("own", "rep"), None, None),
            P(("own", "rep")),
            P(("own", "rep")),
            P(("own", "rep")),
        ),
        out_specs=(P("own", "rep", None, None, None), P("own", None), P("own", None)),
        check_vma=False,
    )
```

```python
import functools
import math

import jax
import jax.numpy as jnp
from jax import lax
from jax.experimental import pallas as pl
from jax.experimental.pallas import tpu as pltpu
from jax.sharding import PartitionSpec as P

SLICES = 2
LANES = 128
headroom = 0.5


SIDE = 4
ROUNDS = (
    ((2, 2),), ((2, 0), (0, 2)), ((2, 1), (0, -1)), ((2, -1), (0, 1)),
    ((1, 2), (-1, 0)), ((-1, 2), (1, 0)), ((1, 1), (-1, -1)), ((1, -1), (-1, 1)),
)


def shifted_layer(my_layer, offset, sign=1):
    dx, dz = offset
    x = lax.rem(my_layer // SIDE + sign * dx + SIDE, SIDE)
    z = lax.rem(my_layer % SIDE + sign * dz + SIDE, SIDE)
    return x * SIDE + z


def fill_slots(live, index_row, layer_row, layers, cap, empty):
    n_select = index_row.shape[1]
    before = lax.broadcasted_iota(jnp.int32, (n_select, n_select), 1)
    after = lax.broadcasted_iota(jnp.int32, (n_select, n_select), 0)
    same = before == after
    layer_col = jnp.sum(jnp.where(same, layer_row, 0), axis=1, keepdims=True)
    index_col = jnp.sum(jnp.where(same, index_row, 0), axis=1, keepdims=True)
    is_live = lax.broadcasted_iota(jnp.int32, (n_select, 1), 0) < live
    earlier = jnp.where(before < after, 1.0, 0.0)
    wanted = lax.broadcasted_iota(jnp.int32, (n_select, LANES), 1)
    matches = jnp.where((layer_col == wanted) & is_live, 1.0, 0.0)
    ranking = jnp.dot(earlier, matches, preferred_element_type=jnp.float32)
    shifted = index_col.astype(jnp.float32) - float(empty)
    rows = []
    for slot in range(cap):
        hit = (ranking == float(slot)) & (matches > 0.5)
        rows.append(jnp.sum(jnp.where(hit, shifted, 0.0), axis=0, keepdims=True) + float(empty))
    return jnp.concatenate(rows, axis=0).astype(jnp.int32)


def kernel(own_n, rep_n, cap, counts_hbm, index_hbm, layer_hbm, pool_ref, codes_ref, steps_ref, err_ref,
           live_ref, index_ref, layer_ref, table, slots, pool_v, stage, send, recv, pk_send, pk_recv, pk_mine, pk_rep,
           st_mine, st_recv, er_send, er_recv, er_mine, er_rep,
           table_sem, small_sem, pool_sem, ssem, rsem, pssem, prsem, tssem, trsem, essem, ersem,
           rpssem, rprsem, ressem, rersem):
    rows, tokens, width = pool_ref.shape
    half = width // SLICES
    flat = tokens * half
    group = LANES // math.gcd(half, LANES)
    period = group * half
    layers = own_n // SLICES
    me = lax.axis_index("own")
    rep = lax.axis_index("rep")
    my_layer = me // SLICES
    my_slice = me % SLICES
    tiles = stage.shape[0]
    denominator = float(own_n * rep_n * cap * tokens)
    pieces = 8
    per_piece = rows // pieces

    small = [
        pltpu.make_async_copy(src, dst, small_sem.at[i])
        for i, (src, dst) in enumerate(((counts_hbm, live_ref), (index_hbm, index_ref), (layer_hbm, layer_ref)))
    ]
    loads = [
        pltpu.make_async_copy(
            pool_ref.at[pl.ds(p * per_piece, per_piece)],
            pool_v.at[pl.ds(p * per_piece, per_piece)],
            pool_sem,
        )
        for p in range(pieces)
    ]

    def peer_of(offset, part, sign=1):
        return shifted_layer(my_layer, offset, sign) * SLICES + lax.rem(my_slice + part, SLICES)

    for load in small + loads:
        load.start()

    order = [((0, 0), 1)] + [(o, part) for o in sorted(sum(ROUNDS, ()), key=lambda o: o[0] != 0) for part in range(SLICES)]
    single = [(o, part) for around in ROUNDS[4:] for part in range(SLICES) for o in around]
    double = [(0, 0)] + [o for around in ROUNDS[:4] for o in around]

    def place(offset, part):
        return order.index((offset, part))

    def mirrored(offset):
        return tuple(v if v == 2 else -v for v in offset)

    gates = [((2, 2), 0), ((2, 0), 0), ((2, 1), 0), ((2, -1), 0)]

    def sends(offset, part):
        return gates.index((offset, part)) if (offset, part) in gates else len(gates)

    def lands(offset, part):
        return double.index(offset) if offset in double else len(double) + single.index((offset, part))

    barrier = pltpu.get_barrier_semaphore()
    for offset in sum(ROUNDS, ()):
        for part in range(SLICES):
            pl.semaphore_signal(barrier, inc=1, device_id={"own": peer_of(offset, part)},
                                device_id_type=pl.DeviceIdType.MESH)
    for part in range(1, SLICES):
        pl.semaphore_signal(barrier, inc=1, device_id={"own": peer_of((0, 0), part)},
                            device_id_type=pl.DeviceIdType.MESH)
    for k in range(1, rep_n):
        pl.semaphore_signal(barrier, inc=1, device_id={"rep": lax.rem(rep + k, rep_n)},
                            device_id_type=pl.DeviceIdType.MESH)
    pool_v[rows] = jnp.zeros((tokens, width), pool_v.dtype)
    for load in small:
        load.wait()
    table[...] = fill_slots(live_ref[0], index_ref[...], layer_ref[...], layers, cap, rows)
    to_scalars = pltpu.make_async_copy(table, slots, table_sem)
    to_scalars.start()
    to_scalars.wait()
    pltpu.make_async_copy(pool_ref, pool_v.at[pl.ds(0, rows)], pool_sem).wait()

    def row_of(layer, c):
        return jnp.minimum(jnp.maximum(slots[c, layer], 0), rows)

    def layer_peak(layer, carry):
        best = jnp.zeros((tokens, width), pool_v.dtype)
        for c in range(cap):
            best = jnp.maximum(best, jnp.abs(pool_v[row_of(layer, c)]))
        top = jnp.max(best.astype(jnp.float32), axis=0, keepdims=True)
        for part in range(SLICES):
            one = top[:, part * half:(part + 1) * half]
            pk_send[layer * SLICES + part] = one
        return carry

    def over_own(src, dst, s_sem, r_sem, peer):
        return pltpu.make_async_remote_copy(
            src_ref=src, dst_ref=dst, send_sem=s_sem, recv_sem=r_sem,
            device_id={"own": peer}, device_id_type=pl.DeviceIdType.MESH)

    def peak_copy(k):
        peer = lax.rem(me + k, own_n)
        return over_own(pk_send.at[peer], pk_recv.at[k - 1], pssem, prsem, peer)

    def step_copy(offset, part):
        near = 0 if offset[0] == 0 else 1
        return over_own(st_mine, st_recv.at[place(offset, part)], tssem, trsem.at[near], peer_of(offset, part))

    def error_copy(offset, part):
        peer = peer_of(offset, part)
        return over_own(er_send.at[peer], er_recv.at[place(offset, part)], essem, ersem, peer)

    def all_own(src, dst, s_sem, r_sem):
        return over_own(src, dst, s_sem, r_sem, lax.rem(me + 1, own_n))

    def block_copy(offset, part, at=None):
        peer = peer_of(offset, part)
        src, dst = send.at[peer], recv.at[me]
        if at is not None:
            span = pl.ds(at * (flat // 2), flat // 2)
            src, dst = send.at[peer, :, span], recv.at[me, :, span]
        return over_own(src, dst, ssem.at[sends(offset, part)], rsem.at[lands(offset, part)], peer)

    def stage_layer(layer):
        for c in range(cap):
            block = pool_v[row_of(layer, c)].astype(jnp.float32)
            for q in range(tiles):
                lo, hi = q * LANES, min(width, (q + 1) * LANES)
                stage[q, c * tokens:(c + 1) * tokens, 0:hi - lo] = block[:, lo:hi]

    def flatten_part(layer, low, high):
        def flatten(i, carry):
            rows_of = [
                jnp.concatenate(
                    [stage[q, pl.ds(i * group + j, cap, stride=tokens), :] for q in range(tiles)], axis=1)
                for j in range(group)
            ]
            for part in range(SLICES):
                joined = jnp.concatenate([r[:, part * half:(part + 1) * half] for r in rows_of], axis=1)
                at = pl.multiple_of(i * period, period)
                send[layer * SLICES + part, :, pl.ds(at, period)] = joined.astype(send.dtype)
            return carry

        lax.fori_loop(low, high, flatten, 0)

    def flatten_layer(layer):
        stage_layer(layer)
        flatten_part(layer, 0, tokens // group)

    def flatten_to(*offsets):
        for offset in offsets:
            flatten_layer(shifted_layer(my_layer, offset))

    def send_to(*offsets):
        for part in range(SLICES):
            for offset in offsets:
                if offset != (0, 0) or part:
                    block_copy(offset, part).start()

    def released(gate):
        all_own(send.at[0], send.at[0], ssem.at[gate], rsem.at[0]).wait_send()

    def over_rep(src, dst, s_sem, r_sem, k):
        return pltpu.make_async_remote_copy(
            src_ref=src, dst_ref=dst, send_sem=s_sem, recv_sem=r_sem,
            device_id={"rep": lax.rem(rep + k, rep_n)}, device_id_type=pl.DeviceIdType.MESH)

    def rep_copy(mine, table, s_sem, r_sem, k):
        return over_rep(mine, table.at[k - 1], s_sem, r_sem, k)

    def wide(row):
        return jnp.broadcast_to(jnp.concatenate([row] * group, axis=1), (cap, period))

    first = shifted_layer(my_layer, (2, 2))
    stage_layer(first)
    flatten_part(first, 0, tokens // group // 2)
    pl.semaphore_wait(barrier, own_n - 1 + rep_n - 1)
    for part in range(SLICES):
        block_copy((2, 2), part, 0).start()
    flatten_part(first, tokens // group // 2, tokens // group)
    for part in range(SLICES):
        block_copy((2, 2), part, 1).start()
    lax.fori_loop(0, layers, layer_peak, 0)
    for k in range(1, own_n):
        peak_copy(k).start()
    for offset in ((2, 0), (2, 1)):
        flatten_to(offset)
        send_to(offset)
    flatten_to((0, 0), (0, 2), (0, -1))
    send_to((0, 0))
    released(0)
    send_to((0, 2))
    flatten_to((0, 1), (2, -1))

    all_own(pk_recv, pk_recv, pssem, prsem).wait_recv()
    best = jnp.maximum(pk_send[me], jnp.max(pk_recv[...], axis=0))
    pk_mine[...] = best
    for k in range(1, rep_n):
        rep_copy(pk_mine, pk_rep, rpssem, rprsem, k).start()
    flatten_to((1, 2), (-1, 0), (-1, 2))
    over_rep(pk_rep, pk_rep, rpssem, rprsem, 1).wait_recv()
    best = jnp.maximum(best, jnp.max(pk_rep[...], axis=0))

    narrow = headroom * jnp.maximum(best, 1.0) / 127.0
    steps_ref[...] = narrow
    st_mine[...] = narrow
    for offset, part in order:
        step_copy(offset, part).start()
    send_to((2, -1))
    inv_wide = wide(1.0 / narrow)
    released(1)
    send_to((0, -1))
    flatten_to((1, 0), (1, 1), (-1, -1), (1, -1), (-1, 1))

    def encode(source, src):
        def one(i, carry):
            at = pl.multiple_of(i * period, period)
            x = source[src, :, pl.ds(at, period)].astype(jnp.float32)
            codes_ref[0, 0, src, :, pl.ds(at, period)] = jnp.clip(x * inv_wide, -127.0, 127.0).astype(codes_ref.dtype)
            return carry
        lax.fori_loop(0, tokens // group, one, 0)

    def landed(offset, part):
        here = recv.at[pl.ds(0, SLICES if offset in double and offset != (0, 0) else 1)]
        all_own(here, here, ssem.at[0], rsem.at[lands(offset, part)]).wait_recv()

    def take(*offsets, parts=range(SLICES)):
        for part in parts:
            for offset in offsets:
                if offset not in double or not part:
                    landed(offset, part)
                encode(recv, peer_of(offset, part, -1))

    def errors(peer, row):
        step_wide, inverse = wide(row), wide(1.0 / row)

        def one(i, total):
            at = pl.multiple_of(i * period, period)
            x = send[peer, :, pl.ds(at, period)].astype(jnp.float32)
            y = jnp.clip(x * inverse, -127.0, 127.0).astype(codes_ref.dtype)
            diff = x - y.astype(jnp.float32) * step_wide
            return total + diff * diff

        total = lax.fori_loop(0, tokens // group, one, jnp.zeros((cap, period), jnp.float32))
        folded = jnp.sum(total, axis=0, keepdims=True)
        return sum(folded[:, j * half:(j + 1) * half] for j in range(1, group)) + folded[:, :half]

    def errors_to(*offsets):
        for offset in offsets:
            for part in range(SLICES):
                if offset != (0, 0) or part:
                    peer = peer_of(offset, part)
                    er_send[peer] = errors(peer, st_recv[place(mirrored(offset), part)])
                    error_copy(offset, part).start()

    def stepped(near):
        first, count = ((0, n_near), (n_near, len(order) - n_near))[near]
        here = st_recv.at[pl.ds(first, count)]
        all_own(here, here, tssem, trsem.at[near]).wait_recv()

    n_near = sum(offset[0] == 0 for offset, _ in order)
    encode(send, me)
    landed((0, 0), 1)
    encode(recv, peer_of((0, 0), 1))
    take((2, 2))
    released(2)
    send_to((0, 1))
    mine = errors(me, narrow)
    stepped(0)
    errors_to((0, 0), (0, 2), (0, 1), (0, -1))
    take((2, 0))
    take((0, 2))
    released(3)
    for around in ROUNDS[4:6]:
        send_to(*around)
    stepped(1)
    errors_to((1, 0), (-1, 0), (2, 0), (1, 1), (-1, -1), (1, -1), (-1, 1), (2, 1), (2, -1), (1, 2), (-1, 2), (2, 2))
    for around in ROUNDS[6:]:
        send_to(*around)
    for around in ROUNDS[2:7]:
        take(*around)
    all_own(er_recv, er_recv, essem, ersem).wait_recv()
    mine = mine + jnp.sum(er_recv[...], axis=0)
    er_mine[...] = mine
    for k in range(1, rep_n):
        rep_copy(er_mine, er_rep, ressem, rersem, k).start()
    take(*ROUNDS[7], parts=(0,))
    over_rep(er_rep.at[pl.ds(0, rep_n - 1)], er_rep.at[pl.ds(0, rep_n - 1)], ressem, rersem, 1).wait_recv()
    er_rep[rep_n - 1] = mine
    whole = er_rep[lax.rem(rep + rep_n - 1, rep_n)]
    for r in range(1, rep_n):
        whole = whole + er_rep[lax.rem(rep + 2 * rep_n - 1 - r, rep_n)]
    err_ref[...] = whole / (narrow * narrow * denominator)
    others = own_n - 1
    all_own(pk_send.at[pl.ds(0, others)], pk_recv, pssem, prsem).wait_send()
    all_own(st_recv, st_recv, tssem, trsem.at[0]).wait_send()
    all_own(er_send.at[pl.ds(0, others)], er_recv, essem, ersem).wait_send()
    over_rep(pk_rep, pk_rep, rpssem, rprsem, 1).wait_send()
    over_rep(er_rep.at[pl.ds(0, rep_n - 1)], pk_rep, ressem, rersem, 1).wait_send()
    take(*ROUNDS[7], parts=(1,))
    rest = send.at[pl.ds(0, others - len(gates))]
    all_own(rest, rest, ssem.at[len(gates)], rsem.at[0]).wait_send()


def write_out(codes_v, steps_v, err_v, codes_ref, steps_ref, err_ref, sems):
    own_n = codes_v.shape[2]
    pieces = 8
    per_piece = own_n // pieces
    for p in range(pieces):
        at = pl.ds(p * per_piece, per_piece)
        pltpu.make_async_copy(codes_v.at[:, :, at], codes_ref.at[:, :, at], sems.at[0]).start()
    moves = [pltpu.make_async_copy(steps_v, steps_ref, sems.at[1]), pltpu.make_async_copy(err_v, err_ref, sems.at[2])]
    for move in moves:
        move.start()
    for move in moves:
        move.wait()
    pltpu.make_async_copy(codes_v, codes_ref, sems.at[0]).wait()


def body(block_pool, sel_index, sel_layer, counts):
    own_n = lax.axis_size("own")
    rep_n = lax.axis_size("rep")
    cap = sel_index.shape[0] // 4
    rows, tokens, width = block_pool.shape
    half = width // SLICES
    flat = tokens * half
    group = LANES // math.gcd(half, LANES)
    period = group * half
    layers = own_n // SLICES
    f32 = jnp.float32
    dma = pltpu.SemaphoreType.DMA
    dtype = block_pool.dtype
    codes, steps, err = pl.pallas_call(
        functools.partial(kernel, own_n, rep_n, cap),
        out_shape=(
            pltpu.VMEM((1, 1, own_n, cap, flat), dtype),
            pltpu.VMEM((1, half), f32),
            pltpu.VMEM((1, half), f32),
        ),
        in_specs=[pl.BlockSpec(memory_space=pltpu.HBM)] * 4,
        out_specs=(
            pl.BlockSpec(memory_space=pltpu.VMEM),
            pl.BlockSpec(memory_space=pltpu.VMEM),
            pl.BlockSpec(memory_space=pltpu.VMEM),
        ),
        scratch_shapes=[
            pltpu.SMEM((1,), jnp.int32),
            pltpu.VMEM((1, sel_index.shape[0]), jnp.int32),
            pltpu.VMEM((1, sel_layer.shape[0]), jnp.int32),
            pltpu.VMEM((cap, LANES), jnp.int32),
            pltpu.SMEM((cap, LANES), jnp.int32),
            pltpu.VMEM((rows + 1, tokens, width), dtype),
            pltpu.VMEM((pl.cdiv(width, LANES), cap * tokens, LANES), f32),
            pltpu.VMEM((own_n, cap, flat), dtype),
            pltpu.VMEM((own_n, cap, flat), dtype),
            pltpu.VMEM((own_n, 1, half), f32),
            pltpu.VMEM((own_n - 1, 1, half), f32),
            pltpu.VMEM((1, half), f32),
            pltpu.VMEM((rep_n - 1, 1, half), f32),
            pltpu.VMEM((1, half), f32),
            pltpu.VMEM((own_n - 1, 1, half), f32),
            pltpu.VMEM((own_n, 1, half), f32),
            pltpu.VMEM((own_n - 1, 1, half), f32),
            pltpu.VMEM((1, half), f32),
            pltpu.VMEM((rep_n, 1, half), f32),
            dma, dma((3,)), dma,
            dma((5,)), dma((24,)), dma, dma, dma, dma((2,)), dma, dma,
            dma, dma, dma, dma,
        ],
        compiler_params=pltpu.CompilerParams(
            collective_id=0, has_side_effects=True, vmem_limit_bytes=(63 * 1024 * 1024 - own_n * cap * flat * 2)),
        name="latent_code",
    )(counts, sel_index[None], sel_layer[None], block_pool)
    hbm = pl.BlockSpec(memory_space=pltpu.HBM)
    return pl.pallas_call(
        write_out,
        out_shape=tuple(jax.ShapeDtypeStruct(x.shape, x.dtype) for x in (codes, steps, err)),
        in_specs=[pl.BlockSpec(memory_space=pltpu.VMEM)] * 3,
        out_specs=(hbm, hbm, hbm),
        scratch_shapes=[dma((3,))],
        compiler_params=pltpu.CompilerParams(vmem_limit_bytes=4 * 1024 * 1024),
        name="write_out",
    )(codes, steps, err)


def solution(mesh):
    return jax.shard_map(
        body,
        mesh=mesh,
        in_specs=(
            P(("own", "rep"), None, None),
            P(("own", "rep")),
            P(("own", "rep")),
            P(("own", "rep")),
        ),
        out_specs=(P("own", "rep", None, None, None), P("own", None), P("own", None)),
        check_vma=False,
    )
```

```python
import functools
import math

import jax
import jax.numpy as jnp
from jax import lax
from jax.experimental import pallas as pl
from jax.experimental.pallas import tpu as pltpu
from jax.sharding import PartitionSpec as P

SLICES = 2
LANES = 128
PIECES = 4
headroom = 0.5


SIDE = 4
ROUNDS = (
    ((2, 2),), ((2, 0), (0, 2)), ((2, 1), (0, -1)), ((2, -1), (0, 1)),
    ((1, 2), (-1, 0)), ((-1, 2), (1, 0)), ((1, 1), (-1, -1)), ((1, -1), (-1, 1)),
)


def shifted_layer(my_layer, offset, sign=1):
    dx, dz = offset
    x = lax.rem(my_layer // SIDE + sign * dx + SIDE, SIDE)
    z = lax.rem(my_layer % SIDE + sign * dz + SIDE, SIDE)
    return x * SIDE + z


def fill_slots(live, index_row, layer_row, layers, cap, empty):
    n_select = index_row.shape[1]
    before = lax.broadcasted_iota(jnp.int32, (n_select, n_select), 1)
    after = lax.broadcasted_iota(jnp.int32, (n_select, n_select), 0)
    same = before == after
    layer_col = jnp.sum(jnp.where(same, layer_row, 0), axis=1, keepdims=True)
    index_col = jnp.sum(jnp.where(same, index_row, 0), axis=1, keepdims=True)
    is_live = lax.broadcasted_iota(jnp.int32, (n_select, 1), 0) < live
    earlier = jnp.where(before < after, 1.0, 0.0)
    wanted = lax.broadcasted_iota(jnp.int32, (n_select, LANES), 1)
    matches = jnp.where((layer_col == wanted) & is_live, 1.0, 0.0)
    ranking = jnp.dot(earlier, matches, preferred_element_type=jnp.float32)
    shifted = index_col.astype(jnp.float32) - float(empty)
    rows = []
    for slot in range(cap):
        hit = (ranking == float(slot)) & (matches > 0.5)
        rows.append(jnp.sum(jnp.where(hit, shifted, 0.0), axis=0, keepdims=True) + float(empty))
    return jnp.concatenate(rows, axis=0).astype(jnp.int32)


def kernel(own_n, rep_n, cap, live_ref, index_hbm, layer_hbm, pool_ref, codes_ref, steps_ref, err_ref,
           index_ref, layer_ref, table, slots, pool_v, stage, send, recv, pk_send, pk_recv, pk_mine, pk_rep,
           st_mine, st_recv, er_send, er_recv, er_mine, er_rep,
           table_sem, small_sem, pool_sem, ssem, rsem, pssem, prsem, tssem, trsem, essem, ersem,
           rpssem, rprsem, ressem, rersem):
    rows, tokens, width = pool_ref.shape
    half = width // SLICES
    flat = tokens * half
    group = LANES // math.gcd(half, LANES)
    period = group * half
    layers = own_n // SLICES
    me = lax.axis_index("own")
    rep = lax.axis_index("rep")
    my_layer = me // SLICES
    my_slice = me % SLICES
    tiles = stage.shape[0]
    denominator = float(own_n * rep_n * cap * tokens)
    pieces = 8
    per_piece = rows // pieces

    small = [
        pltpu.make_async_copy(src, dst, small_sem.at[i])
        for i, (src, dst) in enumerate(((index_hbm, index_ref), (layer_hbm, layer_ref)))
    ]
    loads = [
        pltpu.make_async_copy(
            pool_ref.at[pl.ds(p * per_piece, per_piece)],
            pool_v.at[pl.ds(p * per_piece, per_piece)],
            pool_sem,
        )
        for p in range(pieces)
    ]

    def peer_of(offset, part, sign=1):
        return shifted_layer(my_layer, offset, sign) * SLICES + lax.rem(my_slice + part, SLICES)

    for load in small:
        load.start()

    order = [(o, part) for o in sum(ROUNDS, ()) if o[0] for part in range(SLICES)]
    single = [(o, part) for around in ROUNDS[4:] for part in range(SLICES) for o in around]
    double = [(0, 0)] + [o for around in ROUNDS[:4] for o in around]

    def place(offset, part):
        return order.index((offset, part))

    def mirrored(offset):
        return tuple(v if v == 2 else -v for v in offset)

    gates = [((2, 2), 0), ((2, 0), 0), ((2, 1), 0), ((2, -1), 0)]

    def sends(offset, part):
        return gates.index((offset, part)) if (offset, part) in gates else len(gates)

    def lands(offset, part):
        return double.index(offset) if offset in double else len(double) + single.index((offset, part))

    barrier = pltpu.get_barrier_semaphore()
    for offset in sum(ROUNDS, ()):
        for part in range(SLICES):
            pl.semaphore_signal(barrier, inc=1, device_id={"own": peer_of(offset, part)},
                                device_id_type=pl.DeviceIdType.MESH)
    for part in range(1, SLICES):
        pl.semaphore_signal(barrier, inc=1, device_id={"own": peer_of((0, 0), part)},
                            device_id_type=pl.DeviceIdType.MESH)
    for k in range(1, rep_n):
        pl.semaphore_signal(barrier, inc=1, device_id={"rep": lax.rem(rep + k, rep_n)},
                            device_id_type=pl.DeviceIdType.MESH)
    for load in loads:
        load.start()
    pool_v[rows] = jnp.zeros((tokens, width), pool_v.dtype)
    for load in small:
        load.wait()
    table[...] = fill_slots(live_ref[0], index_ref[...], layer_ref[...], layers, cap, rows)
    to_scalars = pltpu.make_async_copy(table, slots, table_sem)
    to_scalars.start()
    to_scalars.wait()
    pltpu.make_async_copy(pool_ref, pool_v.at[pl.ds(0, rows)], pool_sem).wait()

    def row_of(layer, c):
        return jnp.minimum(jnp.maximum(slots[c, layer], 0), rows)

    def layer_peak(layer, carry):
        best = jnp.zeros((tokens, width), pool_v.dtype)
        for c in range(cap):
            best = jnp.maximum(best, jnp.abs(pool_v[row_of(layer, c)]))
        top = jnp.max(best.astype(jnp.float32), axis=0, keepdims=True)
        for part in range(SLICES):
            one = top[:, part * half:(part + 1) * half]
            pk_send[layer * SLICES + part] = one
        return carry

    def over_own(src, dst, s_sem, r_sem, peer):
        return pltpu.make_async_remote_copy(
            src_ref=src, dst_ref=dst, send_sem=s_sem, recv_sem=r_sem,
            device_id={"own": peer}, device_id_type=pl.DeviceIdType.MESH)

    def peak_copy(k):
        peer = lax.rem(me + k, own_n)
        return over_own(pk_send.at[peer], pk_recv.at[k - 1], pssem, prsem, peer)

    def step_copy(offset, part):
        return over_own(st_mine, st_recv.at[place(offset, part)], tssem, trsem, peer_of(offset, part))

    def error_copy(offset, part):
        peer = peer_of(offset, part)
        return over_own(er_send.at[peer], er_recv.at[place(offset, part)], essem, ersem, peer)

    def all_own(src, dst, s_sem, r_sem):
        return over_own(src, dst, s_sem, r_sem, lax.rem(me + 1, own_n))

    def block_copy(offset, part, at=None):
        peer = peer_of(offset, part)
        src, dst = send.at[peer], recv.at[me]
        if at is not None:
            span = pl.ds(at * (flat // PIECES), flat // PIECES)
            src, dst = send.at[peer, :, span], recv.at[me, :, span]
        return over_own(src, dst, ssem.at[sends(offset, part)], rsem.at[lands(offset, part)], peer)

    def stage_layer(layer):
        for c in range(cap):
            block = pool_v[row_of(layer, c)].astype(jnp.float32)
            for q in range(tiles):
                lo, hi = q * LANES, min(width, (q + 1) * LANES)
                stage[q, c * tokens:(c + 1) * tokens, 0:hi - lo] = block[:, lo:hi]

    def flatten_part(layer, low, high):
        def flatten(i, carry):
            rows_of = [
                jnp.concatenate(
                    [stage[q, pl.ds(i * group + j, cap, stride=tokens), :] for q in range(tiles)], axis=1)
                for j in range(group)
            ]
            for part in range(SLICES):
                joined = jnp.concatenate([r[:, part * half:(part + 1) * half] for r in rows_of], axis=1)
                at = pl.multiple_of(i * period, period)
                send[layer * SLICES + part, :, pl.ds(at, period)] = joined.astype(send.dtype)
            return carry

        lax.fori_loop(low, high, flatten, 0)

    def flatten_layer(layer):
        stage_layer(layer)
        flatten_part(layer, 0, tokens // group)

    def flatten_to(*offsets):
        for offset in offsets:
            flatten_layer(shifted_layer(my_layer, offset))

    def send_to(*offsets):
        for part in range(SLICES):
            for offset in offsets:
                if offset != (0, 0) or part:
                    block_copy(offset, part).start()

    def released(gate):
        all_own(send.at[0], send.at[0], ssem.at[gate], rsem.at[0]).wait_send()

    def over_rep(src, dst, s_sem, r_sem, k):
        return pltpu.make_async_remote_copy(
            src_ref=src, dst_ref=dst, send_sem=s_sem, recv_sem=r_sem,
            device_id={"rep": lax.rem(rep + k, rep_n)}, device_id_type=pl.DeviceIdType.MESH)

    def rep_copy(mine, table, s_sem, r_sem, k):
        return over_rep(mine, table.at[k - 1], s_sem, r_sem, k)

    def wide(row):
        return jnp.broadcast_to(jnp.concatenate([row] * group, axis=1), (cap, period))

    first = shifted_layer(my_layer, (2, 2))
    stage_layer(first)
    for at in range(PIECES):
        flatten_part(first, at * (tokens // group // PIECES), (at + 1) * (tokens // group // PIECES))
        if not at:
            pl.semaphore_wait(barrier, own_n - 1 + rep_n - 1)
        for part in range(SLICES):
            block_copy((2, 2), part, at).start()
    lax.fori_loop(0, layers, layer_peak, 0)
    for k in range(1, own_n):
        peak_copy(k).start()
    for offset in ((2, 0), (2, 1)):
        flatten_to(offset)
        send_to(offset)
    flatten_to((0, 0), (0, 2), (0, -1))
    send_to((0, 0))
    released(0)
    send_to((0, 2))
    flatten_to((0, 1), (2, -1))

    all_own(pk_recv, pk_recv, pssem, prsem).wait_recv()
    best = jnp.maximum(pk_send[me], jnp.max(pk_recv[...], axis=0))
    pk_mine[...] = best
    for k in range(1, rep_n):
        rep_copy(pk_mine, pk_rep, rpssem, rprsem, k).start()
    flatten_to((1, 2), (-1, 0), (-1, 2))
    over_rep(pk_rep, pk_rep, rpssem, rprsem, 1).wait_recv()
    best = jnp.maximum(best, jnp.max(pk_rep[...], axis=0))

    narrow = headroom * jnp.maximum(best, 1.0) / 127.0
    steps_ref[...] = narrow
    st_mine[...] = narrow
    for offset, part in order:
        step_copy(offset, part).start()
    send_to((2, -1))
    inv_wide, step_wide = wide(1.0 / narrow), wide(narrow)
    released(1)
    send_to((0, -1))
    flatten_to((1, 0), (1, 1), (-1, -1), (1, -1), (-1, 1))

    def encode(source, src):
        def one(i, carry):
            at = pl.multiple_of(i * period, period)
            x = source[src, :, pl.ds(at, period)].astype(jnp.float32)
            codes_ref[0, 0, src, :, pl.ds(at, period)] = jnp.clip(x * inv_wide, -127.0, 127.0).astype(codes_ref.dtype)
            return carry
        lax.fori_loop(0, tokens // group, one, 0)

    def encode_and_sum(source, src, total):
        def one(i, total):
            at = pl.multiple_of(i * period, period)
            x = source[src, :, pl.ds(at, period)].astype(jnp.float32)
            y = jnp.clip(x * inv_wide, -127.0, 127.0).astype(codes_ref.dtype)
            codes_ref[0, 0, src, :, pl.ds(at, period)] = y
            diff = x - y.astype(jnp.float32) * step_wide
            return total + diff * diff
        return lax.fori_loop(0, tokens // group, one, total)

    def fold(total):
        row = jnp.sum(total, axis=0, keepdims=True)
        return sum(row[:, j * half:(j + 1) * half] for j in range(1, group)) + row[:, :half]

    def landed(offset, part):
        here = recv.at[pl.ds(0, SLICES if offset in double and offset != (0, 0) else 1)]
        all_own(here, here, ssem.at[0], rsem.at[lands(offset, part)]).wait_recv()

    def take(*offsets, parts=range(SLICES)):
        for part in parts:
            for offset in offsets:
                if offset not in double or not part:
                    landed(offset, part)
                encode(recv, peer_of(offset, part, -1))

    def take_and_sum(total, *offsets):
        for offset in offsets:
            landed(offset, 0)
            for part in range(SLICES):
                total = encode_and_sum(recv, peer_of(offset, part, -1), total)
        return total

    def errors(peer, row):
        peer_step, peer_inverse = wide(row), wide(1.0 / row)

        def one(i, total):
            at = pl.multiple_of(i * period, period)
            x = send[peer, :, pl.ds(at, period)].astype(jnp.float32)
            y = jnp.clip(x * peer_inverse, -127.0, 127.0).astype(codes_ref.dtype)
            diff = x - y.astype(jnp.float32) * peer_step
            return total + diff * diff

        return fold(lax.fori_loop(0, tokens // group, one, jnp.zeros((cap, period), jnp.float32)))

    def errors_to(*offsets):
        for offset in offsets:
            for part in range(SLICES):
                peer = peer_of(offset, part)
                er_send[peer] = errors(peer, st_recv[place(mirrored(offset), part)])
                error_copy(offset, part).start()

    take((2, 2))
    released(2)
    send_to((0, 1))
    total = encode_and_sum(send, me, jnp.zeros((cap, period), jnp.float32))
    landed((0, 0), 1)
    total = encode_and_sum(recv, peer_of((0, 0), 1), total)
    take((2, 0))
    total = take_and_sum(total, (0, 2))
    released(3)
    for around in ROUNDS[4:6]:
        send_to(*around)
    all_own(st_recv, st_recv, tssem, trsem).wait_recv()
    errors_to((1, 0), (-1, 0), (2, 0), (1, 1), (-1, -1), (1, -1), (-1, 1), (2, 1), (2, -1), (1, 2), (-1, 2), (2, 2))
    for around in ROUNDS[6:]:
        send_to(*around)
    take((2, 1))
    take((2, -1))
    for around in ROUNDS[4:7]:
        take(*around)
    mine = fold(take_and_sum(total, (0, -1), (0, 1)))
    all_own(er_recv, er_recv, essem, ersem).wait_recv()
    mine = mine + jnp.sum(er_recv[...], axis=0)
    er_mine[...] = mine
    for k in range(1, rep_n):
        rep_copy(er_mine, er_rep, ressem, rersem, k).start()
    take(*ROUNDS[7], parts=(0,))
    over_rep(er_rep.at[pl.ds(0, rep_n - 1)], er_rep.at[pl.ds(0, rep_n - 1)], ressem, rersem, 1).wait_recv()
    er_rep[rep_n - 1] = mine
    whole = er_rep[lax.rem(rep + rep_n - 1, rep_n)]
    for r in range(1, rep_n):
        whole = whole + er_rep[lax.rem(rep + 2 * rep_n - 1 - r, rep_n)]
    err_ref[...] = whole / (narrow * narrow * denominator)
    others = own_n - 1
    all_own(pk_send.at[pl.ds(0, others)], pk_recv, pssem, prsem).wait_send()
    all_own(st_recv, st_recv, tssem, trsem).wait_send()
    all_own(er_recv, er_recv, essem, ersem).wait_send()
    over_rep(pk_rep, pk_rep, rpssem, rprsem, 1).wait_send()
    over_rep(er_rep.at[pl.ds(0, rep_n - 1)], pk_rep, ressem, rersem, 1).wait_send()
    take(*ROUNDS[7], parts=(1,))
    rest = send.at[pl.ds(0, others - len(gates))]
    all_own(rest, rest, ssem.at[len(gates)], rsem.at[0]).wait_send()


def write_out(codes_v, steps_v, err_v, codes_ref, steps_ref, err_ref, sems):
    own_n = codes_v.shape[2]
    pieces = 8
    per_piece = own_n // pieces
    for p in range(pieces):
        at = pl.ds(p * per_piece, per_piece)
        pltpu.make_async_copy(codes_v.at[:, :, at], codes_ref.at[:, :, at], sems.at[0]).start()
    moves = [pltpu.make_async_copy(steps_v, steps_ref, sems.at[1]), pltpu.make_async_copy(err_v, err_ref, sems.at[2])]
    for move in moves:
        move.start()
    for move in moves:
        move.wait()
    pltpu.make_async_copy(codes_v, codes_ref, sems.at[0]).wait()


def body(block_pool, sel_index, sel_layer, counts):
    own_n = lax.axis_size("own")
    rep_n = lax.axis_size("rep")
    cap = sel_index.shape[0] // 4
    rows, tokens, width = block_pool.shape
    half = width // SLICES
    flat = tokens * half
    group = LANES // math.gcd(half, LANES)
    period = group * half
    layers = own_n // SLICES
    f32 = jnp.float32
    dma = pltpu.SemaphoreType.DMA
    dtype = block_pool.dtype
    codes, steps, err = pl.pallas_call(
        functools.partial(kernel, own_n, rep_n, cap),
        out_shape=(
            pltpu.VMEM((1, 1, own_n, cap, flat), dtype),
            pltpu.VMEM((1, half), f32),
            pltpu.VMEM((1, half), f32),
        ),
        in_specs=[pl.BlockSpec(memory_space=pltpu.SMEM)] + [pl.BlockSpec(memory_space=pltpu.HBM)] * 3,
        out_specs=(
            pl.BlockSpec(memory_space=pltpu.VMEM),
            pl.BlockSpec(memory_space=pltpu.VMEM),
            pl.BlockSpec(memory_space=pltpu.VMEM),
        ),
        scratch_shapes=[
            pltpu.VMEM((1, sel_index.shape[0]), jnp.int32),
            pltpu.VMEM((1, sel_layer.shape[0]), jnp.int32),
            pltpu.VMEM((cap, LANES), jnp.int32),
            pltpu.SMEM((cap, LANES), jnp.int32),
            pltpu.VMEM((rows + 1, tokens, width), dtype),
            pltpu.VMEM((pl.cdiv(width, LANES), cap * tokens, LANES), f32),
            pltpu.VMEM((own_n, cap, flat), dtype),
            pltpu.VMEM((own_n, cap, flat), dtype),
            pltpu.VMEM((own_n, 1, half), f32),
            pltpu.VMEM((own_n - 1, 1, half), f32),
            pltpu.VMEM((1, half), f32),
            pltpu.VMEM((rep_n - 1, 1, half), f32),
            pltpu.VMEM((1, half), f32),
            pltpu.VMEM((own_n - SIDE * SLICES, 1, half), f32),
            pltpu.VMEM((own_n, 1, half), f32),
            pltpu.VMEM((own_n - SIDE * SLICES, 1, half), f32),
            pltpu.VMEM((1, half), f32),
            pltpu.VMEM((rep_n, 1, half), f32),
            dma, dma((2,)), dma,
            dma((5,)), dma((24,)), dma, dma, dma, dma, dma, dma,
            dma, dma, dma, dma,
        ],
        compiler_params=pltpu.CompilerParams(
            collective_id=0, has_side_effects=True, vmem_limit_bytes=(63 * 1024 * 1024 - own_n * cap * flat * 2)),
        name="latent_code",
    )(counts, sel_index[None], sel_layer[None], block_pool)
    hbm = pl.BlockSpec(memory_space=pltpu.HBM)
    return pl.pallas_call(
        write_out,
        out_shape=tuple(jax.ShapeDtypeStruct(x.shape, x.dtype) for x in (codes, steps, err)),
        in_specs=[pl.BlockSpec(memory_space=pltpu.VMEM)] * 3,
        out_specs=(hbm, hbm, hbm),
        scratch_shapes=[dma((3,))],
        compiler_params=pltpu.CompilerParams(vmem_limit_bytes=4 * 1024 * 1024),
        name="write_out",
    )(codes, steps, err)


def solution(mesh):
    return jax.shard_map(
        body,
        mesh=mesh,
        in_specs=(
            P(("own", "rep"), None, None),
            P(("own", "rep")),
            P(("own", "rep")),
            P(("own", "rep")),
        ),
        out_specs=(P("own", "rep", None, None, None), P("own", None), P("own", None)),
        check_vma=False,
    )
```

```python
import functools
import math

import jax
import jax.numpy as jnp
from jax import lax
from jax.experimental import pallas as pl
from jax.experimental.pallas import tpu as pltpu
from jax.sharding import PartitionSpec as P

SLICES = 2
LANES = 128
PIECES = 4
headroom = 0.5


SIDE = 4
ROUNDS = (
    ((2, 2),), ((2, 0), (0, 2)), ((2, 1), (0, -1)), ((2, -1), (0, 1)),
    ((1, 2), (-1, 0)), ((-1, 2), (1, 0)), ((1, 1), (-1, -1)), ((1, -1), (-1, 1)),
)


def shifted_layer(my_layer, offset, sign=1):
    dx, dz = offset
    x = lax.rem(my_layer // SIDE + sign * dx + SIDE, SIDE)
    z = lax.rem(my_layer % SIDE + sign * dz + SIDE, SIDE)
    return x * SIDE + z


def fill_slots(live, index_row, layer_row, layers, cap, empty):
    n_select = index_row.shape[1]
    before = lax.broadcasted_iota(jnp.int32, (n_select, n_select), 1)
    after = lax.broadcasted_iota(jnp.int32, (n_select, n_select), 0)
    same = before == after
    layer_col = jnp.sum(jnp.where(same, layer_row, 0), axis=1, keepdims=True)
    index_col = jnp.sum(jnp.where(same, index_row, 0), axis=1, keepdims=True)
    is_live = lax.broadcasted_iota(jnp.int32, (n_select, 1), 0) < live
    earlier = jnp.where(before < after, 1.0, 0.0)
    wanted = lax.broadcasted_iota(jnp.int32, (n_select, LANES), 1)
    matches = jnp.where((layer_col == wanted) & is_live, 1.0, 0.0)
    ranking = jnp.dot(earlier, matches, preferred_element_type=jnp.float32)
    shifted = index_col.astype(jnp.float32) - float(empty)
    rows = []
    for slot in range(cap):
        hit = (ranking == float(slot)) & (matches > 0.5)
        rows.append(jnp.sum(jnp.where(hit, shifted, 0.0), axis=0, keepdims=True) + float(empty))
    return jnp.concatenate(rows, axis=0).astype(jnp.int32)


def kernel(own_n, rep_n, cap, live_ref, index_hbm, layer_hbm, pool_ref, codes_ref, steps_ref, err_ref,
           index_ref, layer_ref, table, slots, pool_v, stage, send, recv, pk_send, pk_recv, pk_mine, pk_rep,
           st_mine, st_recv, er_send, er_recv, er_mine, er_rep,
           table_sem, small_sem, pool_sem, ssem, rsem, pssem, prsem, tssem, trsem, essem, ersem,
           rpssem, rprsem, ressem, rersem):
    rows, tokens, width = pool_ref.shape
    half = width // SLICES
    flat = tokens * half
    group = LANES // math.gcd(half, LANES)
    period = group * half
    layers = own_n // SLICES
    me = lax.axis_index("own")
    rep = lax.axis_index("rep")
    my_layer = me // SLICES
    my_slice = me % SLICES
    tiles = stage.shape[0]
    denominator = float(own_n * rep_n * cap * tokens)
    pieces = 8
    per_piece = rows // pieces

    small = [
        pltpu.make_async_copy(src, dst, small_sem.at[i])
        for i, (src, dst) in enumerate(((index_hbm, index_ref), (layer_hbm, layer_ref)))
    ]
    loads = [
        pltpu.make_async_copy(
            pool_ref.at[pl.ds(p * per_piece, per_piece)],
            pool_v.at[pl.ds(p * per_piece, per_piece)],
            pool_sem,
        )
        for p in range(pieces)
    ]

    def peer_of(offset, part, sign=1):
        return shifted_layer(my_layer, offset, sign) * SLICES + lax.rem(my_slice + part, SLICES)

    for load in small:
        load.start()

    order = [(o, part) for o in ROUNDS[7] for part in range(SLICES)]
    single = [(o, part) for around in ROUNDS[4:] for part in range(SLICES) for o in around]
    double = [(0, 0)] + [o for around in ROUNDS[:4] for o in around]

    def place(offset, part):
        return order.index((offset, part))

    def mirrored(offset):
        return tuple(v if v == 2 else -v for v in offset)

    gates = [((2, 2), 0), ((2, 0), 0), ((2, 1), 0), ((2, -1), 0)]

    def sends(offset, part):
        return gates.index((offset, part)) if (offset, part) in gates else len(gates)

    def lands(offset, part):
        return double.index(offset) if offset in double else len(double) + single.index((offset, part))

    barrier = pltpu.get_barrier_semaphore()
    for offset in sum(ROUNDS, ()):
        for part in range(SLICES):
            pl.semaphore_signal(barrier, inc=1, device_id={"own": peer_of(offset, part)},
                                device_id_type=pl.DeviceIdType.MESH)
    for part in range(1, SLICES):
        pl.semaphore_signal(barrier, inc=1, device_id={"own": peer_of((0, 0), part)},
                            device_id_type=pl.DeviceIdType.MESH)
    for k in range(1, rep_n):
        pl.semaphore_signal(barrier, inc=1, device_id={"rep": lax.rem(rep + k, rep_n)},
                            device_id_type=pl.DeviceIdType.MESH)
    for load in loads:
        load.start()
    pool_v[rows] = jnp.zeros((tokens, width), pool_v.dtype)
    for load in small:
        load.wait()
    table[...] = fill_slots(live_ref[0], index_ref[...], layer_ref[...], layers, cap, rows)
    to_scalars = pltpu.make_async_copy(table, slots, table_sem)
    to_scalars.start()
    to_scalars.wait()
    pltpu.make_async_copy(pool_ref, pool_v.at[pl.ds(0, rows)], pool_sem).wait()

    def row_of(layer, c):
        return jnp.minimum(jnp.maximum(slots[c, layer], 0), rows)

    def layer_peak(layer, carry):
        best = jnp.zeros((tokens, width), pool_v.dtype)
        for c in range(cap):
            best = jnp.maximum(best, jnp.abs(pool_v[row_of(layer, c)]))
        top = jnp.max(best.astype(jnp.float32), axis=0, keepdims=True)
        for part in range(SLICES):
            one = top[:, part * half:(part + 1) * half]
            pk_send[layer * SLICES + part] = one.astype(pk_send.dtype)
        return carry

    def over_own(src, dst, s_sem, r_sem, peer):
        return pltpu.make_async_remote_copy(
            src_ref=src, dst_ref=dst, send_sem=s_sem, recv_sem=r_sem,
            device_id={"own": peer}, device_id_type=pl.DeviceIdType.MESH)

    def peak_copy(k):
        peer = lax.rem(me + k, own_n)
        return over_own(pk_send.at[peer], pk_recv.at[k - 1], pssem, prsem, peer)

    def step_copy(offset, part):
        return over_own(st_mine, st_recv.at[place(offset, part)], tssem, trsem, peer_of(offset, part))

    def error_copy(offset, part):
        at = place(offset, part)
        return over_own(er_send.at[at], er_recv.at[at], essem, ersem, peer_of(offset, part))

    def all_own(src, dst, s_sem, r_sem):
        return over_own(src, dst, s_sem, r_sem, lax.rem(me + 1, own_n))

    def block_copy(offset, part, at=None):
        peer = peer_of(offset, part)
        src, dst = send.at[peer], recv.at[me]
        if at is not None:
            span = pl.ds(at * (flat // PIECES), flat // PIECES)
            src, dst = send.at[peer, :, span], recv.at[me, :, span]
        return over_own(src, dst, ssem.at[sends(offset, part)], rsem.at[lands(offset, part)], peer)

    def stage_layer(layer):
        for c in range(cap):
            block = pool_v[row_of(layer, c)].astype(jnp.float32)
            for q in range(tiles):
                lo, hi = q * LANES, min(width, (q + 1) * LANES)
                stage[q, c * tokens:(c + 1) * tokens, 0:hi - lo] = block[:, lo:hi]

    def flatten_part(layer, low, high):
        def flatten(i, carry):
            rows_of = [
                jnp.concatenate(
                    [stage[q, pl.ds(i * group + j, cap, stride=tokens), :] for q in range(tiles)], axis=1)
                for j in range(group)
            ]
            for part in range(SLICES):
                joined = jnp.concatenate([r[:, part * half:(part + 1) * half] for r in rows_of], axis=1)
                at = pl.multiple_of(i * period, period)
                send[layer * SLICES + part, :, pl.ds(at, period)] = joined.astype(send.dtype)
            return carry

        lax.fori_loop(low, high, flatten, 0)

    def flatten_layer(layer):
        stage_layer(layer)
        flatten_part(layer, 0, tokens // group)

    def flatten_to(*offsets):
        for offset in offsets:
            flatten_layer(shifted_layer(my_layer, offset))

    def send_to(*offsets):
        for part in range(SLICES):
            for offset in offsets:
                if offset != (0, 0) or part:
                    block_copy(offset, part).start()

    def released(gate):
        all_own(send.at[0], send.at[0], ssem.at[gate], rsem.at[0]).wait_send()

    def over_rep(src, dst, s_sem, r_sem, k):
        return pltpu.make_async_remote_copy(
            src_ref=src, dst_ref=dst, send_sem=s_sem, recv_sem=r_sem,
            device_id={"rep": lax.rem(rep + k, rep_n)}, device_id_type=pl.DeviceIdType.MESH)

    def rep_copy(mine, table, s_sem, r_sem, k):
        return over_rep(mine, table.at[k - 1], s_sem, r_sem, k)

    def wide(row):
        return jnp.broadcast_to(jnp.concatenate([row] * group, axis=1), (cap, period))

    first = shifted_layer(my_layer, (2, 2))
    stage_layer(first)
    for at in range(PIECES):
        flatten_part(first, at * (tokens // group // PIECES), (at + 1) * (tokens // group // PIECES))
        if not at:
            pl.semaphore_wait(barrier, own_n - 1 + rep_n - 1)
        for part in range(SLICES):
            block_copy((2, 2), part, at).start()
    lax.fori_loop(0, layers, layer_peak, 0)
    for k in range(1, own_n):
        peak_copy(k).start()
    for offset in ((2, 0), (2, 1)):
        flatten_to(offset)
        send_to(offset)
    flatten_to((0, 0), (0, 2), (0, -1))
    send_to((0, 0))
    released(0)
    send_to((0, 2))
    flatten_to((0, 1), (2, -1))

    all_own(pk_recv, pk_recv, pssem, prsem).wait_recv()
    best = jnp.maximum(pk_send[me].astype(jnp.float32), jnp.max(pk_recv[...].astype(jnp.float32), axis=0))
    pk_mine[...] = best
    for k in range(1, rep_n):
        rep_copy(pk_mine, pk_rep, rpssem, rprsem, k).start()
    flatten_to((1, 2), (-1, 0), (-1, 2))
    over_rep(pk_rep, pk_rep, rpssem, rprsem, 1).wait_recv()
    best = jnp.maximum(best, jnp.max(pk_rep[...], axis=0))

    narrow = headroom * jnp.maximum(best, 1.0) / 127.0
    steps_ref[...] = narrow
    st_mine[...] = narrow
    for offset, part in order:
        step_copy(offset, part).start()
    send_to((2, -1))
    inv_wide, step_wide = wide(1.0 / narrow), wide(narrow)
    released(1)
    send_to((0, -1))
    flatten_to((1, 0), (1, 1), (-1, -1), (1, -1), (-1, 1))

    def encode(source, src):
        def one(i, carry):
            at = pl.multiple_of(i * period, period)
            x = source[src, :, pl.ds(at, period)].astype(jnp.float32)
            codes_ref[0, 0, src, :, pl.ds(at, period)] = jnp.clip(x * inv_wide, -127.0, 127.0).astype(codes_ref.dtype)
            return carry
        lax.fori_loop(0, tokens // group, one, 0)

    def encode_and_sum(source, src, total):
        def one(i, total):
            at = pl.multiple_of(i * period, period)
            x = source[src, :, pl.ds(at, period)].astype(jnp.float32)
            y = jnp.clip(x * inv_wide, -127.0, 127.0).astype(codes_ref.dtype)
            codes_ref[0, 0, src, :, pl.ds(at, period)] = y
            diff = x - y.astype(jnp.float32) * step_wide
            return total + diff * diff
        return lax.fori_loop(0, tokens // group, one, total)

    def fold(total):
        row = jnp.sum(total, axis=0, keepdims=True)
        return sum(row[:, j * half:(j + 1) * half] for j in range(1, group)) + row[:, :half]

    def landed(offset, part):
        here = recv.at[pl.ds(0, SLICES if offset in double and offset != (0, 0) else 1)]
        all_own(here, here, ssem.at[0], rsem.at[lands(offset, part)]).wait_recv()

    def take(*offsets, parts=range(SLICES)):
        for part in parts:
            for offset in offsets:
                if offset not in double or not part:
                    landed(offset, part)
                encode(recv, peer_of(offset, part, -1))

    def take_and_sum(total, *offsets):
        for part in range(SLICES):
            for offset in offsets:
                if offset not in double or not part:
                    landed(offset, part)
                total = encode_and_sum(recv, peer_of(offset, part, -1), total)
        return total

    def errors(peer, row):
        peer_step, peer_inverse = wide(row), wide(1.0 / row)

        def one(i, total):
            at = pl.multiple_of(i * period, period)
            x = send[peer, :, pl.ds(at, period)].astype(jnp.float32)
            y = jnp.clip(x * peer_inverse, -127.0, 127.0).astype(codes_ref.dtype)
            diff = x - y.astype(jnp.float32) * peer_step
            return total + diff * diff

        return fold(lax.fori_loop(0, tokens // group, one, jnp.zeros((cap, period), jnp.float32)))

    def errors_to(*offsets):
        for offset in offsets:
            for part in range(SLICES):
                er_send[place(offset, part)] = errors(peer_of(offset, part), st_recv[place(mirrored(offset), part)])
                error_copy(offset, part).start()

    total = encode_and_sum(send, me, jnp.zeros((cap, period), jnp.float32))
    released(2)
    send_to((0, 1))
    landed((0, 0), 1)
    total = encode_and_sum(recv, peer_of((0, 0), 1), total)
    total = take_and_sum(total, (2, 2))
    total = take_and_sum(total, (2, 0))
    total = take_and_sum(total, (0, 2))
    released(3)
    for around in ROUNDS[4:6]:
        send_to(*around)
    all_own(st_recv, st_recv, tssem, trsem).wait_recv()
    errors_to(*ROUNDS[7])
    for around in ROUNDS[6:]:
        send_to(*around)
    total = take_and_sum(total, (2, 1))
    total = take_and_sum(total, (2, -1))
    for around in ROUNDS[4:7]:
        total = take_and_sum(total, *around)
    mine = fold(take_and_sum(total, (0, -1), (0, 1)))
    all_own(er_recv, er_recv, essem, ersem).wait_recv()
    mine = mine + jnp.sum(er_recv[...], axis=0)
    er_mine[...] = mine
    for k in range(1, rep_n):
        rep_copy(er_mine, er_rep, ressem, rersem, k).start()
    take(*ROUNDS[7], parts=(0,))
    over_rep(er_rep.at[pl.ds(0, rep_n - 1)], er_rep.at[pl.ds(0, rep_n - 1)], ressem, rersem, 1).wait_recv()
    er_rep[rep_n - 1] = mine
    whole = er_rep[lax.rem(rep + rep_n - 1, rep_n)]
    for r in range(1, rep_n):
        whole = whole + er_rep[lax.rem(rep + 2 * rep_n - 1 - r, rep_n)]
    err_ref[...] = whole / (narrow * narrow * denominator)
    others = own_n - 1
    all_own(pk_send.at[pl.ds(0, others)], pk_recv, pssem, prsem).wait_send()
    all_own(st_recv, st_recv, tssem, trsem).wait_send()
    all_own(er_recv, er_recv, essem, ersem).wait_send()
    over_rep(pk_rep, pk_rep, rpssem, rprsem, 1).wait_send()
    over_rep(er_rep.at[pl.ds(0, rep_n - 1)], pk_rep, ressem, rersem, 1).wait_send()
    take(*ROUNDS[7], parts=(1,))
    rest = send.at[pl.ds(0, others - len(gates))]
    all_own(rest, rest, ssem.at[len(gates)], rsem.at[0]).wait_send()


def write_out(codes_v, steps_v, err_v, codes_ref, steps_ref, err_ref, sems):
    own_n = codes_v.shape[2]
    pieces = 8
    per_piece = own_n // pieces
    for p in range(pieces):
        at = pl.ds(p * per_piece, per_piece)
        pltpu.make_async_copy(codes_v.at[:, :, at], codes_ref.at[:, :, at], sems.at[0]).start()
    moves = [pltpu.make_async_copy(steps_v, steps_ref, sems.at[1]), pltpu.make_async_copy(err_v, err_ref, sems.at[2])]
    for move in moves:
        move.start()
    for move in moves:
        move.wait()
    pltpu.make_async_copy(codes_v, codes_ref, sems.at[0]).wait()


def body(block_pool, sel_index, sel_layer, counts):
    own_n = lax.axis_size("own")
    rep_n = lax.axis_size("rep")
    cap = sel_index.shape[0] // 4
    rows, tokens, width = block_pool.shape
    half = width // SLICES
    flat = tokens * half
    group = LANES // math.gcd(half, LANES)
    period = group * half
    layers = own_n // SLICES
    f32 = jnp.float32
    dma = pltpu.SemaphoreType.DMA
    dtype = block_pool.dtype
    codes, steps, err = pl.pallas_call(
        functools.partial(kernel, own_n, rep_n, cap),
        out_shape=(
            pltpu.VMEM((1, 1, own_n, cap, flat), dtype),
            pltpu.VMEM((1, half), f32),
            pltpu.VMEM((1, half), f32),
        ),
        in_specs=[pl.BlockSpec(memory_space=pltpu.SMEM)] + [pl.BlockSpec(memory_space=pltpu.HBM)] * 3,
        out_specs=(
            pl.BlockSpec(memory_space=pltpu.VMEM),
            pl.BlockSpec(memory_space=pltpu.VMEM),
            pl.BlockSpec(memory_space=pltpu.VMEM),
        ),
        scratch_shapes=[
            pltpu.VMEM((1, sel_index.shape[0]), jnp.int32),
            pltpu.VMEM((1, sel_layer.shape[0]), jnp.int32),
            pltpu.VMEM((cap, LANES), jnp.int32),
            pltpu.SMEM((cap, LANES), jnp.int32),
            pltpu.VMEM((rows + 1, tokens, width), dtype),
            pltpu.VMEM((pl.cdiv(width, LANES), cap * tokens, LANES), f32),
            pltpu.VMEM((own_n, cap, flat), dtype),
            pltpu.VMEM((own_n, cap, flat), dtype),
            pltpu.VMEM((own_n, 1, half), dtype),
            pltpu.VMEM((own_n - 1, 1, half), dtype),
            pltpu.VMEM((1, half), f32),
            pltpu.VMEM((rep_n - 1, 1, half), f32),
            pltpu.VMEM((1, half), f32),
            pltpu.VMEM((len(ROUNDS[7]) * SLICES, 1, half), f32),
            pltpu.VMEM((len(ROUNDS[7]) * SLICES, 1, half), f32),
            pltpu.VMEM((len(ROUNDS[7]) * SLICES, 1, half), f32),
            pltpu.VMEM((1, half), f32),
            pltpu.VMEM((rep_n, 1, half), f32),
            dma, dma((2,)), dma,
            dma((5,)), dma((24,)), dma, dma, dma, dma, dma, dma,
            dma, dma, dma, dma,
        ],
        compiler_params=pltpu.CompilerParams(
            collective_id=0, has_side_effects=True, vmem_limit_bytes=(63 * 1024 * 1024 - own_n * cap * flat * 2)),
        name="latent_code",
    )(counts, sel_index[None], sel_layer[None], block_pool)
    hbm = pl.BlockSpec(memory_space=pltpu.HBM)
    return pl.pallas_call(
        write_out,
        out_shape=tuple(jax.ShapeDtypeStruct(x.shape, x.dtype) for x in (codes, steps, err)),
        in_specs=[pl.BlockSpec(memory_space=pltpu.VMEM)] * 3,
        out_specs=(hbm, hbm, hbm),
        scratch_shapes=[dma((3,))],
        compiler_params=pltpu.CompilerParams(vmem_limit_bytes=4 * 1024 * 1024),
        name="write_out",
    )(codes, steps, err)


def solution(mesh):
    return jax.shard_map(
        body,
        mesh=mesh,
        in_specs=(
            P(("own", "rep"), None, None),
            P(("own", "rep")),
            P(("own", "rep")),
            P(("own", "rep")),
        ),
        out_specs=(P("own", "rep", None, None, None), P("own", None), P("own", None)),
        check_vma=False,
    )
```

```python
import functools
import math

import jax
import jax.numpy as jnp
from jax import lax
from jax.experimental import pallas as pl
from jax.experimental.pallas import tpu as pltpu
from jax.sharding import PartitionSpec as P

SLICES = 2
LANES = 128
PIECES = 8
headroom = 0.5


SIDE = 4
ROUNDS = (
    ((2, 2),), ((2, 0), (0, 2)), ((2, 1), (0, -1)), ((2, -1), (0, 1)),
    ((1, 2), (-1, 0)), ((-1, 2), (1, 0)), ((1, 1), (-1, -1)), ((1, -1), (-1, 1)),
)


def shifted_layer(my_layer, offset, sign=1):
    dx, dz = offset
    x = lax.rem(my_layer // SIDE + sign * dx + SIDE, SIDE)
    z = lax.rem(my_layer % SIDE + sign * dz + SIDE, SIDE)
    return x * SIDE + z


def fill_slots(live, index_row, layer_row, layers, cap, empty):
    n_select = index_row.shape[1]
    before = lax.broadcasted_iota(jnp.int32, (n_select, n_select), 1)
    after = lax.broadcasted_iota(jnp.int32, (n_select, n_select), 0)
    same = before == after
    layer_col = jnp.sum(jnp.where(same, layer_row, 0), axis=1, keepdims=True)
    index_col = jnp.sum(jnp.where(same, index_row, 0), axis=1, keepdims=True)
    is_live = lax.broadcasted_iota(jnp.int32, (n_select, 1), 0) < live
    earlier = jnp.where(before < after, 1.0, 0.0)
    wanted = lax.broadcasted_iota(jnp.int32, (n_select, LANES), 1)
    matches = jnp.where((layer_col == wanted) & is_live, 1.0, 0.0)
    ranking = jnp.dot(earlier, matches, preferred_element_type=jnp.float32)
    shifted = index_col.astype(jnp.float32) - float(empty)
    rows = []
    for slot in range(cap):
        hit = (ranking == float(slot)) & (matches > 0.5)
        rows.append(jnp.sum(jnp.where(hit, shifted, 0.0), axis=0, keepdims=True) + float(empty))
    return jnp.concatenate(rows, axis=0).astype(jnp.int32)


def kernel(own_n, rep_n, cap, live_ref, index_hbm, layer_hbm, pool_ref, codes_ref, steps_ref, err_ref,
           index_ref, layer_ref, table, slots, pool_v, stage, send, recv, pk_send, pk_recv, pk_mine, pk_rep,
           st_mine, st_recv, er_send, er_recv, er_mine, er_rep,
           table_sem, small_sem, pool_sem, ssem, rsem, pssem, prsem, tssem, trsem, essem, ersem,
           rpssem, rprsem, ressem, rersem):
    rows, tokens, width = pool_ref.shape
    half = width // SLICES
    flat = tokens * half
    group = LANES // math.gcd(half, LANES)
    period = group * half
    layers = own_n // SLICES
    me = lax.axis_index("own")
    rep = lax.axis_index("rep")
    my_layer = me // SLICES
    my_slice = me % SLICES
    tiles = stage.shape[0]
    denominator = float(own_n * rep_n * cap * tokens)
    pieces = 8
    per_piece = rows // pieces

    small = [
        pltpu.make_async_copy(src, dst, small_sem.at[i])
        for i, (src, dst) in enumerate(((index_hbm, index_ref), (layer_hbm, layer_ref)))
    ]
    loads = [
        pltpu.make_async_copy(
            pool_ref.at[pl.ds(p * per_piece, per_piece)],
            pool_v.at[pl.ds(p * per_piece, per_piece)],
            pool_sem,
        )
        for p in range(pieces)
    ]

    def peer_of(offset, part, sign=1):
        return shifted_layer(my_layer, offset, sign) * SLICES + lax.rem(my_slice + part, SLICES)

    for load in small:
        load.start()

    order = [(o, part) for o in ROUNDS[7] for part in range(SLICES)]
    single = [(o, part) for around in ROUNDS[7:] for part in range(SLICES) for o in around]
    double = [(0, 0)] + [o for around in ROUNDS[:7] for o in around]

    def place(offset, part):
        return order.index((offset, part))

    def mirrored(offset):
        return tuple(v if v == 2 else -v for v in offset)

    gates = [((2, 2), 0), ((2, 0), 0), ((2, 1), 0), ((2, -1), 0)]

    def sends(offset, part):
        return gates.index((offset, part)) if (offset, part) in gates else len(gates)

    def lands(offset, part):
        return double.index(offset) if offset in double else len(double) + single.index((offset, part))

    barrier = pltpu.get_barrier_semaphore()
    for offset in sum(ROUNDS, ()):
        for part in range(SLICES):
            pl.semaphore_signal(barrier, inc=1, device_id={"own": peer_of(offset, part)},
                                device_id_type=pl.DeviceIdType.MESH)
    for part in range(1, SLICES):
        pl.semaphore_signal(barrier, inc=1, device_id={"own": peer_of((0, 0), part)},
                            device_id_type=pl.DeviceIdType.MESH)
    for k in range(1, rep_n):
        pl.semaphore_signal(barrier, inc=1, device_id={"rep": lax.rem(rep + k, rep_n)},
                            device_id_type=pl.DeviceIdType.MESH)
    for load in loads:
        load.start()
    pool_v[rows] = jnp.zeros((tokens, width), pool_v.dtype)
    for load in small:
        load.wait()
    table[...] = fill_slots(live_ref[0], index_ref[...], layer_ref[...], layers, cap, rows)
    to_scalars = pltpu.make_async_copy(table, slots, table_sem)
    to_scalars.start()
    to_scalars.wait()
    pltpu.make_async_copy(pool_ref, pool_v.at[pl.ds(0, rows)], pool_sem).wait()

    def row_of(layer, c):
        return jnp.minimum(jnp.maximum(slots[c, layer], 0), rows)

    def layer_peak(layer, carry):
        best = jnp.zeros((tokens, width), pool_v.dtype)
        for c in range(cap):
            best = jnp.maximum(best, jnp.abs(pool_v[row_of(layer, c)]))
        top = jnp.max(best.astype(jnp.float32), axis=0, keepdims=True)
        for part in range(SLICES):
            one = top[:, part * half:(part + 1) * half]
            pk_send[layer * SLICES + part] = one.astype(pk_send.dtype)
        return carry

    def over_own(src, dst, s_sem, r_sem, peer):
        return pltpu.make_async_remote_copy(
            src_ref=src, dst_ref=dst, send_sem=s_sem, recv_sem=r_sem,
            device_id={"own": peer}, device_id_type=pl.DeviceIdType.MESH)

    def peak_copy(k):
        peer = lax.rem(me + k, own_n)
        return over_own(pk_send.at[peer], pk_recv.at[k - 1], pssem, prsem, peer)

    def step_copy(offset, part):
        return over_own(st_mine, st_recv.at[place(offset, part)], tssem, trsem, peer_of(offset, part))

    def error_copy(offset, part):
        at = place(offset, part)
        return over_own(er_send.at[at], er_recv.at[at], essem, ersem, peer_of(offset, part))

    def all_own(src, dst, s_sem, r_sem):
        return over_own(src, dst, s_sem, r_sem, lax.rem(me + 1, own_n))

    def block_copy(offset, part, at=None):
        peer = peer_of(offset, part)
        src, dst = send.at[peer], recv.at[me]
        if at is not None:
            span = pl.ds(at * (flat // PIECES), flat // PIECES)
            src, dst = send.at[peer, :, span], recv.at[me, :, span]
        return over_own(src, dst, ssem.at[sends(offset, part)], rsem.at[lands(offset, part)], peer)

    def stage_layer(layer):
        for c in range(cap):
            block = pool_v[row_of(layer, c)].astype(jnp.float32)
            for q in range(tiles):
                lo, hi = q * LANES, min(width, (q + 1) * LANES)
                stage[q, c * tokens:(c + 1) * tokens, 0:hi - lo] = block[:, lo:hi]

    def flatten_part(layer, low, high):
        def flatten(i, carry):
            rows_of = [
                jnp.concatenate(
                    [stage[q, pl.ds(i * group + j, cap, stride=tokens), :] for q in range(tiles)], axis=1)
                for j in range(group)
            ]
            for part in range(SLICES):
                joined = jnp.concatenate([r[:, part * half:(part + 1) * half] for r in rows_of], axis=1)
                at = pl.multiple_of(i * period, period)
                send[layer * SLICES + part, :, pl.ds(at, period)] = joined.astype(send.dtype)
            return carry

        lax.fori_loop(low, high, flatten, 0)

    def flatten_layer(layer):
        stage_layer(layer)
        flatten_part(layer, 0, tokens // group)

    def flatten_to(*offsets):
        for offset in offsets:
            flatten_layer(shifted_layer(my_layer, offset))

    def send_to(*offsets):
        for part in range(SLICES):
            for offset in offsets:
                if offset != (0, 0) or part:
                    block_copy(offset, part).start()

    def released(gate):
        all_own(send.at[0], send.at[0], ssem.at[gate], rsem.at[0]).wait_send()

    def over_rep(src, dst, s_sem, r_sem, k):
        return pltpu.make_async_remote_copy(
            src_ref=src, dst_ref=dst, send_sem=s_sem, recv_sem=r_sem,
            device_id={"rep": lax.rem(rep + k, rep_n)}, device_id_type=pl.DeviceIdType.MESH)

    def rep_copy(mine, table, s_sem, r_sem, k):
        return over_rep(mine, table.at[k - 1], s_sem, r_sem, k)

    def wide(row):
        return jnp.broadcast_to(jnp.concatenate([row] * group, axis=1), (cap, period))

    first = shifted_layer(my_layer, (2, 2))
    stage_layer(first)
    for at in range(PIECES):
        flatten_part(first, at * (tokens // group // PIECES), (at + 1) * (tokens // group // PIECES))
        if not at:
            pl.semaphore_wait(barrier, own_n - 1 + rep_n - 1)
        for part in range(SLICES):
            block_copy((2, 2), part, at).start()
    lax.fori_loop(0, layers, layer_peak, 0)
    for k in range(1, own_n):
        peak_copy(k).start()
    for offset in ((2, 0), (2, 1)):
        flatten_to(offset)
        send_to(offset)
    flatten_to((0, 0), (0, 2), (0, -1))
    send_to((0, 0))
    released(0)
    send_to((0, 2))
    flatten_to((0, 1), (2, -1))

    all_own(pk_recv, pk_recv, pssem, prsem).wait_recv()
    best = jnp.maximum(pk_send[me].astype(jnp.float32), jnp.max(pk_recv[...].astype(jnp.float32), axis=0))
    pk_mine[...] = best
    for k in range(1, rep_n):
        rep_copy(pk_mine, pk_rep, rpssem, rprsem, k).start()
    flatten_to((1, 2), (-1, 0), (-1, 2))
    over_rep(pk_rep, pk_rep, rpssem, rprsem, 1).wait_recv()
    best = jnp.maximum(best, jnp.max(pk_rep[...], axis=0))

    narrow = headroom * jnp.maximum(best, 1.0) / 127.0
    steps_ref[...] = narrow
    st_mine[...] = narrow
    for offset, part in order:
        step_copy(offset, part).start()
    send_to((2, -1))
    inv_wide, step_wide = wide(1.0 / narrow), wide(narrow)
    released(1)
    send_to((0, -1))
    flatten_to((1, 0), (1, 1), (-1, -1), (1, -1), (-1, 1))

    def encode(source, src):
        def one(i, carry):
            at = pl.multiple_of(i * period, period)
            x = source[src, :, pl.ds(at, period)].astype(jnp.float32)
            codes_ref[0, 0, src, :, pl.ds(at, period)] = jnp.clip(x * inv_wide, -127.0, 127.0).astype(codes_ref.dtype)
            return carry
        lax.fori_loop(0, tokens // group, one, 0)

    def encode_and_sum(source, src, total):
        def one(i, total):
            at = pl.multiple_of(i * period, period)
            x = source[src, :, pl.ds(at, period)].astype(jnp.float32)
            y = jnp.clip(x * inv_wide, -127.0, 127.0).astype(codes_ref.dtype)
            codes_ref[0, 0, src, :, pl.ds(at, period)] = y
            diff = x - y.astype(jnp.float32) * step_wide
            return total + diff * diff
        return lax.fori_loop(0, tokens // group, one, total)

    def fold(total):
        row = jnp.sum(total, axis=0, keepdims=True)
        return sum(row[:, j * half:(j + 1) * half] for j in range(1, group)) + row[:, :half]

    def landed(offset, part):
        here = recv.at[pl.ds(0, SLICES if offset in double and offset != (0, 0) else 1)]
        all_own(here, here, ssem.at[0], rsem.at[lands(offset, part)]).wait_recv()

    def take(*offsets, parts=range(SLICES)):
        for part in parts:
            for offset in offsets:
                if offset not in double or not part:
                    landed(offset, part)
                encode(recv, peer_of(offset, part, -1))

    def take_and_sum(total, *offsets):
        for part in range(SLICES):
            for offset in offsets:
                if offset not in double or not part:
                    landed(offset, part)
                total = encode_and_sum(recv, peer_of(offset, part, -1), total)
        return total

    def errors(peer, row):
        peer_step, peer_inverse = wide(row), wide(1.0 / row)

        def one(i, total):
            at = pl.multiple_of(i * period, period)
            x = send[peer, :, pl.ds(at, period)].astype(jnp.float32)
            y = jnp.clip(x * peer_inverse, -127.0, 127.0).astype(codes_ref.dtype)
            diff = x - y.astype(jnp.float32) * peer_step
            return total + diff * diff

        return fold(lax.fori_loop(0, tokens // group, one, jnp.zeros((cap, period), jnp.float32)))

    def errors_to(*offsets):
        for offset in offsets:
            for part in range(SLICES):
                er_send[place(offset, part)] = errors(peer_of(offset, part), st_recv[place(mirrored(offset), part)])
                error_copy(offset, part).start()

    total = encode_and_sum(send, me, jnp.zeros((cap, period), jnp.float32))
    landed((0, 0), 1)
    total = encode_and_sum(recv, peer_of((0, 0), 1), total)
    total = take_and_sum(total, (2, 2))
    total = take_and_sum(total, (2, 0))
    released(2)
    send_to((0, 1))
    total = take_and_sum(total, (0, 2))
    released(3)
    for around in ROUNDS[4:6]:
        send_to(*around)
    all_own(st_recv, st_recv, tssem, trsem).wait_recv()
    errors_to(*ROUNDS[7])
    for around in ROUNDS[6:]:
        send_to(*around)
    total = take_and_sum(total, (2, 1))
    total = take_and_sum(total, (2, -1))
    for around in ROUNDS[4:7]:
        total = take_and_sum(total, *around)
    mine = fold(take_and_sum(total, (0, -1), (0, 1)))
    all_own(er_recv, er_recv, essem, ersem).wait_recv()
    mine = mine + jnp.sum(er_recv[...], axis=0)
    er_mine[...] = mine
    for k in range(1, rep_n):
        rep_copy(er_mine, er_rep, ressem, rersem, k).start()
    take(*ROUNDS[7], parts=(0,))
    over_rep(er_rep.at[pl.ds(0, rep_n - 1)], er_rep.at[pl.ds(0, rep_n - 1)], ressem, rersem, 1).wait_recv()
    er_rep[rep_n - 1] = mine
    whole = er_rep[lax.rem(rep + rep_n - 1, rep_n)]
    for r in range(1, rep_n):
        whole = whole + er_rep[lax.rem(rep + 2 * rep_n - 1 - r, rep_n)]
    err_ref[...] = whole / (narrow * narrow * denominator)
    others = own_n - 1
    all_own(pk_send.at[pl.ds(0, others)], pk_recv, pssem, prsem).wait_send()
    all_own(st_recv, st_recv, tssem, trsem).wait_send()
    all_own(er_recv, er_recv, essem, ersem).wait_send()
    over_rep(pk_rep, pk_rep, rpssem, rprsem, 1).wait_send()
    over_rep(er_rep.at[pl.ds(0, rep_n - 1)], pk_rep, ressem, rersem, 1).wait_send()
    take(*ROUNDS[7], parts=(1,))
    rest = send.at[pl.ds(0, others - len(gates))]
    all_own(rest, rest, ssem.at[len(gates)], rsem.at[0]).wait_send()


def write_out(codes_v, steps_v, err_v, codes_ref, steps_ref, err_ref, sems):
    own_n = codes_v.shape[2]
    pieces = 8
    per_piece = own_n // pieces
    for p in range(pieces):
        at = pl.ds(p * per_piece, per_piece)
        pltpu.make_async_copy(codes_v.at[:, :, at], codes_ref.at[:, :, at], sems.at[0]).start()
    moves = [pltpu.make_async_copy(steps_v, steps_ref, sems.at[1]), pltpu.make_async_copy(err_v, err_ref, sems.at[2])]
    for move in moves:
        move.start()
    for move in moves:
        move.wait()
    pltpu.make_async_copy(codes_v, codes_ref, sems.at[0]).wait()


def body(block_pool, sel_index, sel_layer, counts):
    own_n = lax.axis_size("own")
    rep_n = lax.axis_size("rep")
    cap = sel_index.shape[0] // 4
    rows, tokens, width = block_pool.shape
    half = width // SLICES
    flat = tokens * half
    group = LANES // math.gcd(half, LANES)
    period = group * half
    layers = own_n // SLICES
    f32 = jnp.float32
    dma = pltpu.SemaphoreType.DMA
    dtype = block_pool.dtype
    codes, steps, err = pl.pallas_call(
        functools.partial(kernel, own_n, rep_n, cap),
        out_shape=(
            pltpu.VMEM((1, 1, own_n, cap, flat), dtype),
            pltpu.VMEM((1, half), f32),
            pltpu.VMEM((1, half), f32),
        ),
        in_specs=[pl.BlockSpec(memory_space=pltpu.SMEM)] + [pl.BlockSpec(memory_space=pltpu.HBM)] * 3,
        out_specs=(
            pl.BlockSpec(memory_space=pltpu.VMEM),
            pl.BlockSpec(memory_space=pltpu.VMEM),
            pl.BlockSpec(memory_space=pltpu.VMEM),
        ),
        scratch_shapes=[
            pltpu.VMEM((1, sel_index.shape[0]), jnp.int32),
            pltpu.VMEM((1, sel_layer.shape[0]), jnp.int32),
            pltpu.VMEM((cap, LANES), jnp.int32),
            pltpu.SMEM((cap, LANES), jnp.int32),
            pltpu.VMEM((rows + 1, tokens, width), dtype),
            pltpu.VMEM((pl.cdiv(width, LANES), cap * tokens, LANES), f32),
            pltpu.VMEM((own_n, cap, flat), dtype),
            pltpu.VMEM((own_n, cap, flat), dtype),
            pltpu.VMEM((own_n, 1, half), dtype),
            pltpu.VMEM((own_n - 1, 1, half), dtype),
            pltpu.VMEM((1, half), f32),
            pltpu.VMEM((rep_n - 1, 1, half), f32),
            pltpu.VMEM((1, half), f32),
            pltpu.VMEM((len(ROUNDS[7]) * SLICES, 1, half), f32),
            pltpu.VMEM((len(ROUNDS[7]) * SLICES, 1, half), f32),
            pltpu.VMEM((len(ROUNDS[7]) * SLICES, 1, half), f32),
            pltpu.VMEM((1, half), f32),
            pltpu.VMEM((rep_n, 1, half), f32),
            dma, dma((2,)), dma,
            dma((5,)), dma((18,)), dma, dma, dma, dma, dma, dma,
            dma, dma, dma, dma,
        ],
        compiler_params=pltpu.CompilerParams(
            collective_id=0, has_side_effects=True, vmem_limit_bytes=(63 * 1024 * 1024 - own_n * cap * flat * 2)),
        name="latent_code",
    )(counts, sel_index[None], sel_layer[None], block_pool)
    hbm = pl.BlockSpec(memory_space=pltpu.HBM)
    return pl.pallas_call(
        write_out,
        out_shape=tuple(jax.ShapeDtypeStruct(x.shape, x.dtype) for x in (codes, steps, err)),
        in_specs=[pl.BlockSpec(memory_space=pltpu.VMEM)] * 3,
        out_specs=(hbm, hbm, hbm),
        scratch_shapes=[dma((3,))],
        compiler_params=pltpu.CompilerParams(vmem_limit_bytes=4 * 1024 * 1024),
        name="write_out",
    )(codes, steps, err)


def solution(mesh):
    return jax.shard_map(
        body,
        mesh=mesh,
        in_specs=(
            P(("own", "rep"), None, None),
            P(("own", "rep")),
            P(("own", "rep")),
            P(("own", "rep")),
        ),
        out_specs=(P("own", "rep", None, None, None), P("own", None), P("own", None)),
        check_vma=False,
    )
```

```python
import functools
import math

import jax
import jax.numpy as jnp
from jax import lax
from jax.experimental import pallas as pl
from jax.experimental.pallas import tpu as pltpu
from jax.sharding import PartitionSpec as P

SLICES = 2
LANES = 128
PIECES = 8
headroom = 0.5


SIDE = 4
ROUNDS = (
    ((2, 2),), ((2, 0), (0, 2)), ((2, 1), (0, -1)), ((2, -1), (0, 1)),
    ((1, 2), (-1, 0)), ((-1, 2), (1, 0)), ((1, 1), (-1, -1)), ((1, -1), (-1, 1)),
)


def shifted_layer(my_layer, offset, sign=1):
    dx, dz = offset
    x = lax.rem(my_layer // SIDE + sign * dx + SIDE, SIDE)
    z = lax.rem(my_layer % SIDE + sign * dz + SIDE, SIDE)
    return x * SIDE + z


def fill_slots(live, index_row, layer_row, layers, cap, empty):
    n_select = index_row.shape[1]
    before = lax.broadcasted_iota(jnp.int32, (n_select, n_select), 1)
    after = lax.broadcasted_iota(jnp.int32, (n_select, n_select), 0)
    same = before == after
    layer_col = jnp.sum(jnp.where(same, layer_row, 0), axis=1, keepdims=True)
    index_col = jnp.sum(jnp.where(same, index_row, 0), axis=1, keepdims=True)
    is_live = lax.broadcasted_iota(jnp.int32, (n_select, 1), 0) < live
    earlier = jnp.where(before < after, 1.0, 0.0)
    wanted = lax.broadcasted_iota(jnp.int32, (n_select, LANES), 1)
    matches = jnp.where((layer_col == wanted) & is_live, 1.0, 0.0)
    ranking = jnp.dot(earlier, matches, preferred_element_type=jnp.float32)
    shifted = index_col.astype(jnp.float32) - float(empty)
    rows = []
    for slot in range(cap):
        hit = (ranking == float(slot)) & (matches > 0.5)
        rows.append(jnp.sum(jnp.where(hit, shifted, 0.0), axis=0, keepdims=True) + float(empty))
    return jnp.concatenate(rows, axis=0).astype(jnp.int32)


def kernel(own_n, rep_n, cap, live_ref, index_hbm, layer_hbm, pool_ref, codes_ref, steps_ref, err_ref,
           index_ref, layer_ref, table, slots, pool_v, stage, send, recv, pk_send, pk_recv, pk_mine, pk_rep,
           st_mine, st_recv, er_send, er_recv, er_mine, er_rep,
           table_sem, small_sem, pool_sem, ssem, rsem, pssem, prsem, tssem, trsem, essem, ersem,
           rpssem, rprsem, ressem, rersem):
    rows, tokens, width = pool_ref.shape
    half = width // SLICES
    flat = tokens * half
    group = LANES // math.gcd(half, LANES)
    period = group * half
    layers = own_n // SLICES
    me = lax.axis_index("own")
    rep = lax.axis_index("rep")
    my_layer = me // SLICES
    my_slice = me % SLICES
    tiles = stage.shape[0]
    denominator = float(own_n * rep_n * cap * tokens)
    pieces = 8
    per_piece = rows // pieces

    small = [
        pltpu.make_async_copy(src, dst, small_sem.at[i])
        for i, (src, dst) in enumerate(((index_hbm, index_ref), (layer_hbm, layer_ref)))
    ]
    loads = [
        pltpu.make_async_copy(
            pool_ref.at[pl.ds(p * per_piece, per_piece)],
            pool_v.at[pl.ds(p * per_piece, per_piece)],
            pool_sem,
        )
        for p in range(pieces)
    ]

    def peer_of(offset, part, sign=1):
        return shifted_layer(my_layer, offset, sign) * SLICES + lax.rem(my_slice + part, SLICES)

    for load in small:
        load.start()

    order = [(o, part) for o in ROUNDS[7] for part in range(SLICES)]
    single = [(o, part) for around in ROUNDS[7:] for part in range(SLICES) for o in around]
    double = [(0, 0)] + [o for around in ROUNDS[:7] for o in around]

    def place(offset, part):
        return order.index((offset, part))

    def mirrored(offset):
        return tuple(v if v == 2 else -v for v in offset)

    gates = [((2, 2), 0), ((2, 0), 0), ((2, 1), 0), ((2, -1), 0)]

    def sends(offset, part):
        return gates.index((offset, part)) if (offset, part) in gates else len(gates)

    def lands(offset, part):
        return double.index(offset) if offset in double else len(double) + single.index((offset, part))

    barrier = pltpu.get_barrier_semaphore()
    for offset in sum(ROUNDS, ()):
        for part in range(SLICES):
            pl.semaphore_signal(barrier, inc=1, device_id={"own": peer_of(offset, part)},
                                device_id_type=pl.DeviceIdType.MESH)
    for part in range(1, SLICES):
        pl.semaphore_signal(barrier, inc=1, device_id={"own": peer_of((0, 0), part)},
                            device_id_type=pl.DeviceIdType.MESH)
    for k in range(1, rep_n):
        pl.semaphore_signal(barrier, inc=1, device_id={"rep": lax.rem(rep + k, rep_n)},
                            device_id_type=pl.DeviceIdType.MESH)
    for load in loads:
        load.start()
    pool_v[rows] = jnp.zeros((tokens, width), pool_v.dtype)
    for load in small:
        load.wait()
    table[...] = fill_slots(live_ref[0], index_ref[...], layer_ref[...], layers, cap, rows)
    to_scalars = pltpu.make_async_copy(table, slots, table_sem)
    to_scalars.start()
    to_scalars.wait()
    pltpu.make_async_copy(pool_ref, pool_v.at[pl.ds(0, rows)], pool_sem).wait()

    def row_of(layer, c):
        return jnp.minimum(jnp.maximum(slots[c, layer], 0), rows)

    def layer_peak(layer, carry):
        best = jnp.zeros((tokens, width), pool_v.dtype)
        for c in range(cap):
            best = jnp.maximum(best, jnp.abs(pool_v[row_of(layer, c)]))
        top = jnp.max(best.astype(jnp.float32), axis=0, keepdims=True)
        for part in range(SLICES):
            one = top[:, part * half:(part + 1) * half]
            pk_send[layer * SLICES + part] = one.astype(pk_send.dtype)
        return carry

    def over_own(src, dst, s_sem, r_sem, peer):
        return pltpu.make_async_remote_copy(
            src_ref=src, dst_ref=dst, send_sem=s_sem, recv_sem=r_sem,
            device_id={"own": peer}, device_id_type=pl.DeviceIdType.MESH)

    def peak_copy(k):
        peer = lax.rem(me + k, own_n)
        return over_own(pk_send.at[peer], pk_recv.at[k - 1], pssem, prsem, peer)

    def step_copy(offset, part):
        return over_own(st_mine, st_recv.at[place(offset, part)], tssem, trsem, peer_of(offset, part))

    def error_copy(offset, part):
        at = place(offset, part)
        return over_own(er_send.at[at], er_recv.at[at], essem, ersem, peer_of(offset, part))

    def all_own(src, dst, s_sem, r_sem):
        return over_own(src, dst, s_sem, r_sem, lax.rem(me + 1, own_n))

    def block_copy(offset, part, at=None):
        peer = peer_of(offset, part)
        src, dst = send.at[peer], recv.at[me]
        if at is not None:
            span = pl.ds(at * (flat // PIECES), flat // PIECES)
            src, dst = send.at[peer, :, span], recv.at[me, :, span]
        return over_own(src, dst, ssem.at[sends(offset, part)], rsem.at[lands(offset, part)], peer)

    def stage_layer(layer):
        for c in range(cap):
            block = pool_v[row_of(layer, c)].astype(jnp.float32)
            for q in range(tiles):
                lo, hi = q * LANES, min(width, (q + 1) * LANES)
                stage[q, c * tokens:(c + 1) * tokens, 0:hi - lo] = block[:, lo:hi]

    def flatten_part(layer, low, high):
        def flatten(i, carry):
            rows_of = [
                jnp.concatenate(
                    [stage[q, pl.ds(i * group + j, cap, stride=tokens), :] for q in range(tiles)], axis=1)
                for j in range(group)
            ]
            for part in range(SLICES):
                joined = jnp.concatenate([r[:, part * half:(part + 1) * half] for r in rows_of], axis=1)
                at = pl.multiple_of(i * period, period)
                send[layer * SLICES + part, :, pl.ds(at, period)] = joined.astype(send.dtype)
            return carry

        lax.fori_loop(low, high, flatten, 0)

    def flatten_layer(layer):
        stage_layer(layer)
        flatten_part(layer, 0, tokens // group)

    def flatten_to(*offsets):
        for offset in offsets:
            flatten_layer(shifted_layer(my_layer, offset))

    def send_to(*offsets):
        for part in range(SLICES):
            for offset in offsets:
                if offset != (0, 0) or part:
                    block_copy(offset, part).start()

    def released(gate):
        all_own(send.at[0], send.at[0], ssem.at[gate], rsem.at[0]).wait_send()

    def over_rep(src, dst, s_sem, r_sem, k):
        return pltpu.make_async_remote_copy(
            src_ref=src, dst_ref=dst, send_sem=s_sem, recv_sem=r_sem,
            device_id={"rep": lax.rem(rep + k, rep_n)}, device_id_type=pl.DeviceIdType.MESH)

    def rep_copy(mine, table, s_sem, r_sem, k):
        return over_rep(mine, table.at[k - 1], s_sem, r_sem, k)

    def wide(row):
        return jnp.broadcast_to(jnp.concatenate([row] * group, axis=1), (cap, period))

    first = shifted_layer(my_layer, (2, 2))
    stage_layer(first)
    for at in range(PIECES):
        flatten_part(first, at * (tokens // group // PIECES), (at + 1) * (tokens // group // PIECES))
        if not at:
            pl.semaphore_wait(barrier, own_n - 1 + rep_n - 1)
        for part in range(SLICES):
            block_copy((2, 2), part, at).start()
    lax.fori_loop(0, layers, layer_peak, 0)
    for k in range(1, own_n):
        peak_copy(k).start()
    for offset in ((2, 0), (2, 1)):
        flatten_to(offset)
        send_to(offset)
    flatten_to((0, 0), (0, 2), (0, -1))
    send_to((0, 0))
    released(0)
    send_to((0, 2))
    flatten_to((0, 1), (2, -1))

    all_own(pk_recv, pk_recv, pssem, prsem).wait_recv()
    best = jnp.maximum(pk_send[me].astype(jnp.float32), jnp.max(pk_recv[...].astype(jnp.float32), axis=0))
    pk_mine[...] = best
    for k in range(1, rep_n):
        rep_copy(pk_mine, pk_rep, rpssem, rprsem, k).start()
    flatten_to((1, 2), (-1, 0), (-1, 2))
    over_rep(pk_rep, pk_rep, rpssem, rprsem, 1).wait_recv()
    best = jnp.maximum(best, jnp.max(pk_rep[...], axis=0))

    narrow = headroom * jnp.maximum(best, 1.0) / 127.0
    steps_ref[...] = narrow
    st_mine[...] = narrow
    for offset, part in order:
        step_copy(offset, part).start()
    send_to((2, -1))
    inv_wide, step_wide = wide(1.0 / narrow), wide(narrow)
    released(1)
    send_to((0, -1))
    flatten_to((1, 0), (1, 1), (-1, -1), (1, -1), (-1, 1))

    def encode(source, src):
        def one(i, carry):
            at = pl.multiple_of(i * period, period)
            x = source[src, :, pl.ds(at, period)].astype(jnp.float32)
            codes_ref[0, 0, src, :, pl.ds(at, period)] = jnp.clip(x * inv_wide, -127.0, 127.0).astype(codes_ref.dtype)
            return carry
        lax.fori_loop(0, tokens // group, one, 0, unroll=4)

    def encode_and_sum(source, src, total):
        def one(i, total):
            at = pl.multiple_of(i * period, period)
            x = source[src, :, pl.ds(at, period)].astype(jnp.float32)
            y = jnp.clip(x * inv_wide, -127.0, 127.0).astype(codes_ref.dtype)
            codes_ref[0, 0, src, :, pl.ds(at, period)] = y
            diff = x - y.astype(jnp.float32) * step_wide
            return total + diff * diff
        return lax.fori_loop(0, tokens // group, one, total)

    def fold(total):
        row = jnp.sum(total, axis=0, keepdims=True)
        return sum(row[:, j * half:(j + 1) * half] for j in range(1, group)) + row[:, :half]

    def landed(offset, part):
        here = recv.at[pl.ds(0, SLICES if offset in double and offset != (0, 0) else 1)]
        all_own(here, here, ssem.at[0], rsem.at[lands(offset, part)]).wait_recv()

    def take(*offsets, parts=range(SLICES)):
        for part in parts:
            for offset in offsets:
                if offset not in double or not part:
                    landed(offset, part)
                encode(recv, peer_of(offset, part, -1))

    def take_and_sum(total, *offsets):
        for part in range(SLICES):
            for offset in offsets:
                if offset not in double or not part:
                    landed(offset, part)
                total = encode_and_sum(recv, peer_of(offset, part, -1), total)
        return total

    def errors(peer, row):
        peer_step, peer_inverse = wide(row), wide(1.0 / row)

        def one(i, total):
            at = pl.multiple_of(i * period, period)
            x = send[peer, :, pl.ds(at, period)].astype(jnp.float32)
            y = jnp.clip(x * peer_inverse, -127.0, 127.0).astype(codes_ref.dtype)
            diff = x - y.astype(jnp.float32) * peer_step
            return total + diff * diff

        return fold(lax.fori_loop(0, tokens // group, one, jnp.zeros((cap, period), jnp.float32)))

    def errors_to(*offsets):
        for offset in offsets:
            for part in range(SLICES):
                er_send[place(offset, part)] = errors(peer_of(offset, part), st_recv[place(mirrored(offset), part)])
                error_copy(offset, part).start()

    total = encode_and_sum(send, me, jnp.zeros((cap, period), jnp.float32))
    landed((0, 0), 1)
    total = encode_and_sum(recv, peer_of((0, 0), 1), total)
    total = take_and_sum(total, (2, 2))
    total = take_and_sum(total, (2, 0))
    released(2)
    send_to((0, 1))
    total = take_and_sum(total, (0, 2))
    released(3)
    for around in ROUNDS[4:6]:
        send_to(*around)
    all_own(st_recv, st_recv, tssem, trsem).wait_recv()
    errors_to(*ROUNDS[7])
    for around in ROUNDS[6:]:
        send_to(*around)
    total = take_and_sum(total, (2, 1))
    total = take_and_sum(total, (2, -1))
    for around in ROUNDS[4:7]:
        total = take_and_sum(total, *around)
    mine = fold(take_and_sum(total, (0, -1), (0, 1)))
    all_own(er_recv, er_recv, essem, ersem).wait_recv()
    mine = mine + jnp.sum(er_recv[...], axis=0)
    er_mine[...] = mine
    for k in range(1, rep_n):
        rep_copy(er_mine, er_rep, ressem, rersem, k).start()
    take(*ROUNDS[7], parts=(0,))
    over_rep(er_rep.at[pl.ds(0, rep_n - 1)], er_rep.at[pl.ds(0, rep_n - 1)], ressem, rersem, 1).wait_recv()
    er_rep[rep_n - 1] = mine
    whole = er_rep[lax.rem(rep + rep_n - 1, rep_n)]
    for r in range(1, rep_n):
        whole = whole + er_rep[lax.rem(rep + 2 * rep_n - 1 - r, rep_n)]
    err_ref[...] = whole / (narrow * narrow * denominator)
    others = own_n - 1
    all_own(pk_send.at[pl.ds(0, others)], pk_recv, pssem, prsem).wait_send()
    all_own(st_recv, st_recv, tssem, trsem).wait_send()
    all_own(er_recv, er_recv, essem, ersem).wait_send()
    over_rep(pk_rep, pk_rep, rpssem, rprsem, 1).wait_send()
    over_rep(er_rep.at[pl.ds(0, rep_n - 1)], pk_rep, ressem, rersem, 1).wait_send()
    take(*ROUNDS[7], parts=(1,))
    rest = send.at[pl.ds(0, others - len(gates))]
    all_own(rest, rest, ssem.at[len(gates)], rsem.at[0]).wait_send()


def write_out(codes_v, steps_v, err_v, codes_ref, steps_ref, err_ref, sems):
    own_n = codes_v.shape[2]
    pieces = 8
    per_piece = own_n // pieces
    for p in range(pieces):
        at = pl.ds(p * per_piece, per_piece)
        pltpu.make_async_copy(codes_v.at[:, :, at], codes_ref.at[:, :, at], sems.at[0]).start()
    moves = [pltpu.make_async_copy(steps_v, steps_ref, sems.at[1]), pltpu.make_async_copy(err_v, err_ref, sems.at[2])]
    for move in moves:
        move.start()
    for move in moves:
        move.wait()
    pltpu.make_async_copy(codes_v, codes_ref, sems.at[0]).wait()


def body(block_pool, sel_index, sel_layer, counts):
    own_n = lax.axis_size("own")
    rep_n = lax.axis_size("rep")
    cap = sel_index.shape[0] // 4
    rows, tokens, width = block_pool.shape
    half = width // SLICES
    flat = tokens * half
    group = LANES // math.gcd(half, LANES)
    period = group * half
    layers = own_n // SLICES
    f32 = jnp.float32
    dma = pltpu.SemaphoreType.DMA
    dtype = block_pool.dtype
    codes, steps, err = pl.pallas_call(
        functools.partial(kernel, own_n, rep_n, cap),
        out_shape=(
            pltpu.VMEM((1, 1, own_n, cap, flat), dtype),
            pltpu.VMEM((1, half), f32),
            pltpu.VMEM((1, half), f32),
        ),
        in_specs=[pl.BlockSpec(memory_space=pltpu.SMEM)] + [pl.BlockSpec(memory_space=pltpu.HBM)] * 3,
        out_specs=(
            pl.BlockSpec(memory_space=pltpu.VMEM),
            pl.BlockSpec(memory_space=pltpu.VMEM),
            pl.BlockSpec(memory_space=pltpu.VMEM),
        ),
        scratch_shapes=[
            pltpu.VMEM((1, sel_index.shape[0]), jnp.int32),
            pltpu.VMEM((1, sel_layer.shape[0]), jnp.int32),
            pltpu.VMEM((cap, LANES), jnp.int32),
            pltpu.SMEM((cap, LANES), jnp.int32),
            pltpu.VMEM((rows + 1, tokens, width), dtype),
            pltpu.VMEM((pl.cdiv(width, LANES), cap * tokens, LANES), f32),
            pltpu.VMEM((own_n, cap, flat), dtype),
            pltpu.VMEM((own_n, cap, flat), dtype),
            pltpu.VMEM((own_n, 1, half), dtype),
            pltpu.VMEM((own_n - 1, 1, half), dtype),
            pltpu.VMEM((1, half), f32),
            pltpu.VMEM((rep_n - 1, 1, half), f32),
            pltpu.VMEM((1, half), f32),
            pltpu.VMEM((len(ROUNDS[7]) * SLICES, 1, half), f32),
            pltpu.VMEM((len(ROUNDS[7]) * SLICES, 1, half), f32),
            pltpu.VMEM((len(ROUNDS[7]) * SLICES, 1, half), f32),
            pltpu.VMEM((1, half), f32),
            pltpu.VMEM((rep_n, 1, half), f32),
            dma, dma((2,)), dma,
            dma((5,)), dma((18,)), dma, dma, dma, dma, dma, dma,
            dma, dma, dma, dma,
        ],
        compiler_params=pltpu.CompilerParams(
            collective_id=0, has_side_effects=True, vmem_limit_bytes=(63 * 1024 * 1024 - own_n * cap * flat * 2)),
        name="latent_code",
    )(counts, sel_index[None], sel_layer[None], block_pool)
    hbm = pl.BlockSpec(memory_space=pltpu.HBM)
    return pl.pallas_call(
        write_out,
        out_shape=tuple(jax.ShapeDtypeStruct(x.shape, x.dtype) for x in (codes, steps, err)),
        in_specs=[pl.BlockSpec(memory_space=pltpu.VMEM)] * 3,
        out_specs=(hbm, hbm, hbm),
        scratch_shapes=[dma((3,))],
        compiler_params=pltpu.CompilerParams(vmem_limit_bytes=4 * 1024 * 1024),
        name="write_out",
    )(codes, steps, err)


def solution(mesh):
    return jax.shard_map(
        body,
        mesh=mesh,
        in_specs=(
            P(("own", "rep"), None, None),
            P(("own", "rep")),
            P(("own", "rep")),
            P(("own", "rep")),
        ),
        out_specs=(P("own", "rep", None, None, None), P("own", None), P("own", None)),
        check_vma=False,
    )
```
